256 devices in a mesh: tile: 64 (over x, z, core), lev: 4 (over y).
Axes of the slice: x: 4, y: 4, z: 8, core: 2. Of those that a mesh axis runs over, the one named last changes fastest.
Arguments:
- mixing: float32 [3, 64, 262144], P(None, 'lev', 'tile'), may hold values from 0.05 to 3
- density: float32 [64, 262144], P('lev', 'tile'), may hold values from 0.4 to 1.2
- routes: int32 [262144, 1], P('tile'), may hold values from 0 to 63; in each aligned block of 4096 rows (0 to 4095, 4096 to 8191, ...) at most 128 rows name the same one
- beam_weight: float32 [64, 168, 64], P('tile'), may hold values from 0.001 to 0.06
- gate_adjoint: float32 [168, 524288], P('lev', 'tile'), may hold values from -6 to 6
Outputs:
- gate_values: float32 [168, 524288], P('lev', 'tile')
- increments: float32 [3, 64, 262144], P(None, 'lev', 'tile')
The draws below stay inside these ranges and needn't reach their ends.
Inputs may be any that keep to these rules, and one draw needn't show every extreme that they name: `routes`: each column names the site that observes it; the columns of one tile index send at most 128 columns to one site, and exactly 128 to some site.
All inputs are finite; a program needn't handle non-finite values.
Results may differ from the reference program's by a relative error of at most 0.00007.
Values sent between devices are 32-bit elements; how exact they have to be, the bound alone decides.
A program may use at most 64 MiB of HBM per device.

```python
import math
import jax
import jax.numpy as jnp
import numpy as np
from jax import lax

COL_DEV = 4096
LEV = 64
GATE_COL = 168
SITES = 64
CAP = 128
COLS = 262144
SLOTS = 524288
N_TILE = 64


def levels(stream_key, extent, shards, low, high):
    def one(axis_at, parts):
        steps = jax.random.uniform(jax.random.fold_in(jax.random.fold_in(stream_key, 6), axis_at), (parts,), jnp.float32, low / len(shards), high / len(shards))
        return jnp.repeat(jnp.exp(steps), extent[axis_at] // parts).reshape((-1,) + (1,) * (len(extent) - axis_at - 1))

    factor_of = one(*shards[0])
    for cut in shards[1:]:
        factor_of = factor_of * one(*cut)
    return factor_of


def deal_out(own_key, own, number, rows, number_of, top, most, lean):
    order = jax.random.permutation(own_key, number_of)
    crowded, ordinary = shares(number_of, rows * top, most, lean, True), shares(number_of, rows * top, most, lean, False)
    places = jnp.arange(number_of)

    def named(lengths, turn):
        used = int((lengths > 0).sum())
        fixed = max(1, used // 4)
        moved = fixed + (places - fixed + turn * (used - fixed)) % max(1, number_of - fixed)
        return jnp.zeros((number_of,), jnp.int32).at[order[jnp.where(places < fixed, places, moved)]].set(jnp.asarray(lengths, jnp.int32))

    lengths = jnp.where(number % 4 == 0, named(crowded, number // 4), named(ordinary, number - number // 4 - 1))
    mixed = jax.random.permutation(jax.random.fold_in(own, 3), number_of)
    source_of, receiver = mixed[0:number_of // 2 * 2:2], mixed[1:number_of // 2 * 2:2]
    room = jnp.minimum(lengths[source_of] - 1, most - lengths[receiver]) // 2
    room = jnp.where((source_of == order[0]) | (receiver == order[0]) | (lengths[receiver] == 0), 0, jnp.maximum(room, 0))
    moved = jax.random.randint(jax.random.fold_in(own, 4), (number_of // 2,), 0, 1 << 20) % (room + 1)
    lengths = lengths.at[source_of].add(-moved).at[receiver].add(moved)
    items = jnp.searchsorted(jnp.cumsum(lengths), jnp.arange(rows * top), side="right").astype(jnp.int32)
    grid = items.reshape(top, rows).T
    grid = grid[jax.random.permutation(jax.random.fold_in(own, 1), rows)]
    turn = jax.random.randint(jax.random.fold_in(own, 2), (rows, 1), 0, top)
    return jnp.take_along_axis(grid, (jnp.arange(top)[None, :] + turn) % top, axis=1)


def shares(amount, total, most, lean, full):
    weights = [(1 << 20) // math.isqrt(grade ** lean) + 1 for grade in range(1, amount + 1)]
    largest = most if full else min(most, max(-(-total // amount), total * weights[0] // sum(weights)))
    least = 1 if total - largest >= amount - 1 else 0
    given, surplus = [largest] + [least] * (amount - 1), total - largest - least * (amount - 1)
    while surplus > 0:
        movable = [i for i in range(1, amount) if given[i] < largest] or [i for i in range(1, amount) if given[i] < most]
        pool, left = sum([weights[i] for i in movable]), surplus
        for i in movable:
            addition = min(most - given[i], max(1, left * weights[i] // pool), surplus)
            given[i] = given[i] + addition
            surplus = surplus - addition
    return np.array(given)


def normal_values(rng, shape, deviation, bound, cuts=(), kind=jnp.bfloat16):
    loudness = levels(rng, shape, cuts, -0.22, 0.18) if cuts else 1.0
    result = jax.random.normal(rng, shape, jnp.float32) * deviation * loudness
    return jnp.minimum(jnp.maximum(result, -bound), bound).astype(kind)


def setup_inputs(seed: int = 0) -> dict:
    splits = jax.random.split(jax.random.key(seed), 6)
    mixing = jnp.clip(jnp.exp(math.log(3.0) - 4.0943445 * jax.random.uniform(splits[0], (3, LEV, COLS), jnp.float32) ** levels(splits[0], (3, LEV, COLS), ((1, 4), (2, 64)), -0.2, 0.2)), 0.05, 3.0)
    density = jnp.clip(jnp.exp(math.log(1.2) - 1.0986123 * jax.random.uniform(splits[1], (LEV, COLS), jnp.float32) ** levels(splits[1], (LEV, COLS), ((0, 4), (1, 64)), -0.2, 0.2)), 0.4, 1.2)
    routes_keys = jax.random.split(jax.random.fold_in(splits[2], 1), COLS // COL_DEV)
    routes_turns = jax.random.permutation(jax.random.fold_in(splits[2], 3), COLS // COL_DEV)
    routes = jax.vmap(lambda own, number: deal_out(jax.random.fold_in(splits[2], 2), own, number, COL_DEV, N_TILE, 1, CAP, 2))(routes_keys, routes_turns).reshape((COLS, 1))
    beam_weight = jnp.clip(jnp.exp(math.log(0.06) - 4.0943445 * jax.random.uniform(splits[3], (SITES, GATE_COL, LEV), jnp.float32) ** levels(splits[3], (SITES, GATE_COL, LEV), ((0, 64),), -0.2, 0.2)), 0.001, 0.06)
    gate_adjoint = normal_values(splits[4], (GATE_COL, SLOTS), 1.0, 6.0, ((0, 4), (1, 64)), jnp.float32)
    return {"mixing": mixing, "density": density, "routes": routes, "beam_weight": beam_weight, "gate_adjoint": gate_adjoint}


coefficients = (3.63, 0.96, 1.98)
exponents = (1.75, 1.66, 1.75)


def reflect(mixing, density):
    summed = jnp.zeros(density.shape, jnp.float32)
    slopes = []
    for species in range(3):
        scaled = density * mixing[species]
        powered = coefficients[species] * jnp.exp(exponents[species] * jnp.log(scaled))
        summed = summed + powered
        slopes.append(exponents[species] * powered / mixing[species])
    return summed, jnp.stack(slopes)


def reference(mixing, density, routes, beam_weight, gate_adjoint):
    tile_count = N_TILE
    capacity = 2 * COL_DEV // tile_count
    slot_total = tile_count * capacity
    reflectivity, slopes = reflect(mixing, density)
    target = routes[:, 0].reshape(tile_count, COL_DEV).astype(jnp.int32)
    onehot = (target[:, :, None] == jnp.arange(tile_count, dtype=jnp.int32)[None, None, :]).astype(jnp.int32)
    ranking = jnp.sum((jnp.cumsum(onehot, axis=1) - onehot) * onehot, axis=2)
    source = jnp.arange(tile_count, dtype=jnp.int32)[:, None]
    position = (target * slot_total + source * capacity + ranking).reshape(-1).astype(jnp.int32)
    site_columns = jnp.zeros((LEV, tile_count * slot_total), jnp.float32).at[:, position].set(reflectivity)
    gate_values = jnp.einsum("dgl,ldk->gdk", beam_weight, site_columns.reshape(LEV, tile_count, slot_total),
                             precision=lax.Precision.HIGHEST).reshape(GATE_COL, tile_count * slot_total)
    site_adjoint = jnp.einsum("dgl,gdk->ldk", beam_weight, gate_adjoint.reshape(GATE_COL, tile_count, slot_total),
                              precision=lax.Precision.HIGHEST).reshape(LEV, tile_count * slot_total)
    increments = slopes * site_adjoint[:, position][None]
    return gate_values, increments
```

```python
import jax
import jax.numpy as jnp
from jax import lax
from jax.experimental import pallas as pl
from jax.experimental.pallas import tpu as pltpu
from jax.sharding import PartitionSpec as P

coefficients = (3.63, 0.96, 1.98)
exponents = (1.75, 1.66, 1.75)

MESH = pl.DeviceIdType.MESH
F32 = jnp.float32
BF16 = jnp.bfloat16

NX, NZ, NC = 4, 8, 2
LEVS = 4
TILES = NX * NZ * NC
PAIRS = NX * NZ
CHUNKS = 4
PC = PAIRS // CHUNKS
HALF = PC // 2
COLS = 4096
LD = 16
LEV = 64
CAP = 128
GR = 42


def split2(value):
    hi = value.astype(BF16)
    lo = (value - hi.astype(F32)).astype(BF16)
    return hi, lo


def dot(a, b, dims=((1,), (0,))):
    return lax.dot_general(a, b, (dims, ((), ())), preferred_element_type=F32)


def shift_of(kp):
    dzi = kp // NX
    dx = kp % NX
    dz = ((dzi + 1) // 2) * (2 * (dzi % 2) - 1)
    return dx, dz


def kernel(
    mixing_hbm, density_hbm, routes_hbm, weight_hbm, adjoint_hbm,
    gate_hbm, incr_hbm,
    mixing, density, target, weight, adjoint, gate, incr,
    slopes, parts, onehot, prefix, ranks1h, lhs, out_blocks,
    partial, rs1, rs2, final, back, cols, restored,
    in_sem, out_sem, a2a_send, a2a_recv, bk_send, bk_recv,
    rs1_send, rs1_recv, rs2_send, rs2_recv, ag1_send, ag1_recv, ag2_send, ag2_recv,
):
    tile = lax.axis_index("tile")
    lev = lax.axis_index("lev")
    core = tile % NC
    zz = (tile // NC) % NZ
    xx = tile // (NC * NZ)
    right = (lev + 1) % LEVS
    left = (lev + 3) % LEVS
    across = (lev + 2) % LEVS

    def pair_plus(kp):
        dx, dz = shift_of(kp)
        return ((xx + dx) % NX) * NZ + (zz + dz + NZ) % NZ

    def pair_minus(kp):
        dx, dz = shift_of(kp)
        return ((xx - dx + NX) % NX) * NZ + (zz - dz + NZ) % NZ

    loads = [
        pltpu.make_async_copy(weight_hbm.at[0], weight, in_sem.at[0]),
        pltpu.make_async_copy(adjoint_hbm, adjoint, in_sem.at[1]),
        pltpu.make_async_copy(routes_hbm, target, in_sem.at[2]),
        pltpu.make_async_copy(density_hbm, density, in_sem.at[3]),
        pltpu.make_async_copy(mixing_hbm, mixing, in_sem.at[4]),
    ]
    for load in loads:
        load.start()

    barrier = pltpu.get_barrier_semaphore()

    @pl.loop(1, TILES)
    def _(k):
        pl.semaphore_signal(
            barrier, inc=1, device_id={"tile": (tile + k) % TILES}, device_id_type=MESH
        )

    for peer in (left, right):
        pl.semaphore_signal(barrier, inc=1, device_id={"lev": peer}, device_id_type=MESH)

    loads[0].wait()
    rows = jnp.zeros((GR, LEV), F32)
    for k in range(LEVS):
        rows = jnp.where(lev == k, weight[GR * k : GR * (k + 1), :], rows)
    rows_hi, rows_lo = split2(rows)
    loads[1].wait()

    @pl.loop(0, PAIRS)
    def _(kp):
        at = pl.multiple_of(pair_plus(kp) * 2 * CAP, 2 * CAP)
        g_hi, g_lo = split2(adjoint[:, pl.ds(at, 2 * CAP)])
        tn = ((0,), (0,))
        part = dot(rows_hi, g_hi, tn) + dot(rows_hi, g_lo, tn) + dot(rows_lo, g_hi, tn)
        for k in range(LEVS):
            for c in range(NC):
                partial[k, kp * NC + c] = part[LD * k : LD * (k + 1), CAP * c : CAP * (c + 1)]

    pl.semaphore_wait(barrier, TILES - 1 + 2)

    def lev_copy(src, dst, send, recv, peer):
        return pltpu.make_async_remote_copy(
            src_ref=src, dst_ref=dst, send_sem=send, recv_sem=recv,
            device_id={"lev": peer}, device_id_type=MESH,
        )

    def rs1_copy(c, way):
        at = c * PC + way * HALF
        return lev_copy(
            partial.at[across, pl.ds(at * NC, HALF * NC)], rs1.at[way, c],
            rs1_send.at[way, c], rs1_recv.at[way, c], (right, left)[way],
        )

    def rs2_copy(c, way):
        peer = (right, left)[way]
        return lev_copy(
            partial.at[peer, pl.ds(c * PC * NC, PC * NC)], rs2.at[way, c],
            rs2_send.at[way, c], rs2_recv.at[way, c], peer,
        )

    def ag1_copy(c, way):
        here = cols.at[lev, pl.ds(c * PC * NC, PC * NC)]
        return lev_copy(
            here, here, ag1_send.at[way, c], ag1_recv.at[way, c], (right, left)[way]
        )

    def ag2_copy(c, way):
        here = cols.at[(left, right)[way], pl.ds((c * PC + way * HALF) * NC, HALF * NC)]
        return lev_copy(
            here, here, ag2_send.at[way, c], ag2_recv.at[way, c], (right, left)[way]
        )

    def rs_first(c):
        for way in range(2):
            rs1_copy(c, way).start()

    def rs_second(c):
        for way in range(2):
            rs1_copy(c, way).wait_recv()
            peer = (right, left)[way]
            at = pl.ds((c * PC + way * HALF) * NC, HALF * NC)
            partial[peer, at] = partial[peer, at] + rs1[way, c]
        for way in range(2):
            rs2_copy(c, way).start()

    def back_copy(kp, c, cs):
        return pltpu.make_async_remote_copy(
            src_ref=final.at[kp * NC + cs], dst_ref=back.at[kp * NC + core],
            send_sem=bk_send, recv_sem=bk_recv.at[c],
            device_id={"tile": pair_plus(kp) * NC + cs}, device_id_type=MESH,
        )

    def out_copy(kp, c, cd):
        return pltpu.make_async_remote_copy(
            src_ref=out_blocks.at[kp * NC + cd], dst_ref=cols.at[lev, kp * NC + core],
            send_sem=a2a_send, recv_sem=a2a_recv.at[c],
            device_id={"tile": pair_minus(kp) * NC + cd}, device_id_type=MESH,
        )

    def exchange(copy_of, c):
        if c == 0:
            copy_of(0, 0, 1 - core).start()

        @pl.loop(c * PC + (1 if c == 0 else 0), (c + 1) * PC)
        def _(kp):
            for other in range(NC):
                copy_of(kp, c, other).start()

    def blocks(buf, count, send, recv):
        some = buf.at[pl.ds(0, count)]
        return pltpu.make_async_remote_copy(
            src_ref=some, dst_ref=some, send_sem=send, recv_sem=recv,
            device_id={"lev": right}, device_id_type=MESH,
        )

    def in_chunk(c):
        return PC * NC - (1 if c == 0 else 0)

    def rs_final(c):
        for way in range(2):
            rs2_copy(c, way).wait_recv()
        at = pl.ds(c * PC * NC, PC * NC)
        final[at] = partial[lev, at] + rs2[0, c] + rs2[1, c]

    for c in range(CHUNKS):
        rs_first(c)

    loads[2].wait()
    for j in range(COLS // CAP):
        names = lax.broadcasted_iota(jnp.int32, (TILES, CAP), 0)
        onehot[TILES * j : TILES * (j + 1), :] = jnp.where(
            target[:, CAP * j : CAP * (j + 1)] == names, 1.0, 0.0
        ).astype(BF16)
    upto = jnp.where(
        lax.broadcasted_iota(jnp.int32, (CAP, 2 * CAP), 0)
        < lax.broadcasted_iota(jnp.int32, (CAP, 2 * CAP), 1),
        1.0, 0.0,
    ).astype(BF16)
    prefix[...] = dot(onehot[...], upto)
    carry = jnp.zeros((TILES, CAP), F32)
    slot = lax.broadcasted_iota(jnp.int32, (CAP, CAP), 0).astype(F32)
    for j in range(COLS // CAP):
        at = slice(TILES * j, TILES * (j + 1))
        mine = onehot[at, :].astype(F32) * (prefix[at, :CAP] + carry)
        rank = jnp.sum(mine, axis=0, keepdims=True)
        ranks1h[:, CAP * j : CAP * (j + 1)] = jnp.where(rank == slot, 1.0, 0.0).astype(BF16)
        carry = carry + prefix[at, CAP:]

    rs_second(0)

    loads[3].wait()
    loads[4].wait()
    wide = 512

    @pl.loop(0, COLS // wide)
    def _(j):
        at = pl.ds(pl.multiple_of(j * wide, wide), wide)
        dens = density[:, at]
        summed = jnp.zeros((LD, wide), F32)
        for species in range(3):
            mix = mixing[species, :, at]
            powered = coefficients[species] * jnp.exp(exponents[species] * jnp.log(dens * mix))
            summed = summed + powered
            slopes[species, :, at] = exponents[species] * powered / mix
        hi, lo = split2(summed)
        parts[0, :, at] = hi
        parts[1, :, at] = lo

    rs_second(1)

    def scatter(c):
        @pl.loop(0, PC)
        def _(i):
            pair = pair_minus(c * PC + i)
            for cd in range(NC):
                named = jnp.broadcast_to(target[...], (LD, COLS)) == pair * NC + cd
                mask = jnp.where(named, 1.0, 0.0).astype(BF16)
                at = pl.ds(pl.multiple_of((i * NC + cd) * LD, LD), LD)
                lhs[at, :COLS] = mask * parts[0]
                lhs[at, COLS:] = mask * parts[1]

        nt = ((1,), (1,))
        placed = dot(lhs[:, :COLS], ranks1h[...], nt) + dot(lhs[:, COLS:], ranks1h[...], nt)
        for i in range(PC):
            for cd in range(NC):
                at = (i * NC + cd) * LD
                out_blocks[(c * PC + i) * NC + cd] = placed[at : at + LD]
        if c == 0:
            cols[lev, core] = out_blocks[core]

    for c in range(CHUNKS):
        scatter(c)
        exchange(out_copy, c)
        if c < 2:
            rs_second(c + 2)
        else:
            rs_final(c - 2)
    exchange(back_copy, 0)
    exchange(back_copy, 1)

    def ag_first(c):
        blocks(out_blocks, in_chunk(c), a2a_send, a2a_recv.at[c]).wait_recv()
        for way in range(2):
            ag1_copy(c, way).start()

    def ag_second(c):
        for way in range(2):
            ag1_copy(c, way).wait_recv()
        for way in range(2):
            ag2_copy(c, way).start()

    def gates(c):
        for way in range(2):
            ag2_copy(c, way).wait_recv()

        @pl.loop(c * PC, (c + 1) * PC)
        def _(kp):
            both = [cols[:, kp * NC + cs].reshape(LEV, CAP) for cs in range(NC)]
            x_hi, x_lo = split2(jnp.concatenate(both, axis=1))
            at = pl.multiple_of(pair_plus(kp) * 2 * CAP, 2 * CAP)
            gate[:, pl.ds(at, 2 * CAP)] = (
                dot(rows_hi, x_hi) + dot(rows_hi, x_lo) + dot(rows_lo, x_hi)
            )

    def gather(c):
        blocks(final, in_chunk(c), bk_send, bk_recv.at[c]).wait_recv()
        if c == 0:
            back[core] = final[core]
        span = PC * NC * LD
        b_hi, b_lo = split2(back[c * PC * NC : (c + 1) * PC * NC].reshape(span, CAP))
        lhs[:, :CAP] = b_hi
        lhs[:, CAP : 2 * CAP] = b_lo

        @pl.loop(0, COLS // wide)
        def _(j):
            at = pl.ds(pl.multiple_of(j * wide, wide), wide)
            pick = ranks1h[:, at]
            spread = dot(lhs[:, : 2 * CAP], jnp.concatenate([pick, pick], axis=0))
            names = jnp.broadcast_to(target[:, at], (LD, wide))
            if c == 0:
                total = jnp.zeros((LD, wide), F32)
            else:
                total = restored[:, at]
            for i in range(PC):
                pair = pair_minus(c * PC + i)
                for cd in range(NC):
                    mine = spread[(i * NC + cd) * LD : (i * NC + cd + 1) * LD]
                    total = total + jnp.where(names == pair * NC + cd, mine, 0.0)
            if c < CHUNKS - 1:
                restored[:, at] = total
            else:
                for species in range(3):
                    incr[species, :, at] = slopes[species, :, at] * total

    ag_first(0)
    rs_final(2)
    exchange(back_copy, 2)
    ag_first(1)
    ag_second(0)
    rs_final(3)
    exchange(back_copy, 3)
    ag_first(2)
    ag_second(1)
    gates(0)
    gather(0)
    ag_first(3)
    ag_second(2)
    gates(1)
    gather(1)
    ag_second(3)
    gates(2)
    gather(2)
    gather(3)
    inc_out = pltpu.make_async_copy(incr, incr_hbm, out_sem.at[0])
    inc_out.start()
    gates(3)
    gate_out = pltpu.make_async_copy(gate, gate_hbm, out_sem.at[1])
    gate_out.start()

    for c in range(CHUNKS):
        for way in range(2):
            for copy in (rs1_copy, rs2_copy, ag1_copy, ag2_copy):
                copy(c, way).wait_send()
    blocks(out_blocks, TILES - 1, a2a_send, a2a_recv.at[0]).wait_send()
    blocks(final, TILES - 1, bk_send, bk_recv.at[0]).wait_send()
    inc_out.wait()
    gate_out.wait()


def per_device(mixing, density, routes, beam_weight, gate_adjoint):
    dma = pltpu.SemaphoreType.DMA
    block = (LD, CAP)
    per_way = (2, CHUNKS)
    return pl.pallas_call(
        kernel,
        out_shape=(
            jax.ShapeDtypeStruct((GR, TILES * CAP), F32),
            jax.ShapeDtypeStruct((3, LD, COLS), F32),
        ),
        in_specs=[pl.BlockSpec(memory_space=pl.ANY)] * 5,
        out_specs=[pl.BlockSpec(memory_space=pl.ANY)] * 2,
        scratch_shapes=[
            pltpu.VMEM((3, LD, COLS), F32),
            pltpu.VMEM((LD, COLS), F32),
            pltpu.VMEM((1, COLS), jnp.int32),
            pltpu.VMEM((GR * LEVS, LEV), F32),
            pltpu.VMEM((GR, TILES * CAP), F32),
            pltpu.VMEM((GR, TILES * CAP), F32),
            pltpu.VMEM((3, LD, COLS), F32),
            pltpu.VMEM((3, LD, COLS), F32),
            pltpu.VMEM((2, LD, COLS), BF16),
            pltpu.VMEM((TILES * COLS // CAP, CAP), BF16),
            pltpu.VMEM((TILES * COLS // CAP, 2 * CAP), F32),
            pltpu.VMEM((CAP, COLS), BF16),
            pltpu.VMEM((PC * NC * LD, 2 * COLS), BF16),
            pltpu.VMEM((TILES, *block), F32),
            pltpu.VMEM((LEVS, TILES, *block), F32),
            pltpu.VMEM((2, CHUNKS, HALF * NC, *block), F32),
            pltpu.VMEM((2, CHUNKS, PC * NC, *block), F32),
            pltpu.VMEM((TILES, *block), F32),
            pltpu.VMEM((TILES, *block), F32),
            pltpu.VMEM((LEVS, TILES, *block), F32),
            pltpu.VMEM((LD, COLS), F32),
            dma((5,)), dma((2,)), dma, dma((CHUNKS,)), dma, dma((CHUNKS,)),
            dma(per_way), dma(per_way), dma(per_way), dma(per_way),
            dma(per_way), dma(per_way), dma(per_way), dma(per_way),
        ],
        compiler_params=pltpu.CompilerParams(
            collective_id=0, has_side_effects=True, vmem_limit_bytes=48 * 1024 * 1024
        ),
    )(mixing, density, routes.reshape(1, COLS), beam_weight, gate_adjoint)


def solution(mesh):
    return jax.shard_map(
        per_device,
        mesh=mesh,
        in_specs=(
            P(None, "lev", "tile"),
            P("lev", "tile"),
            P("tile", None),
            P("tile", None, None),
            P("lev", "tile"),
        ),
        out_specs=(P("lev", "tile"), P(None, "lev", "tile")),
        check_vma=False,
    )
```

```python
import jax
import jax.numpy as jnp
from jax import lax
from jax.experimental import pallas as pl
from jax.experimental.pallas import tpu as pltpu
from jax.sharding import PartitionSpec as P

coefficients = (3.63, 0.96, 1.98)
exponents = (1.75, 1.66, 1.75)

MESH = pl.DeviceIdType.MESH
F32 = jnp.float32
BF16 = jnp.bfloat16

NX, NZ, NC = 4, 8, 2
LEVS = 4
TILES = NX * NZ * NC
PAIRS = NX * NZ
CHUNKS = 4
PC = PAIRS // CHUNKS
HALF = PC // 2
COLS = 4096
LD = 16
LEV = 64
CAP = 128
GR = 42


def split2(value):
    hi = value.astype(BF16)
    lo = (value - hi.astype(F32)).astype(BF16)
    return hi, lo


def dot(a, b, dims=((1,), (0,))):
    return lax.dot_general(a, b, (dims, ((), ())), preferred_element_type=F32)


def shift_of(kp):
    dzi = kp // NX
    dx = kp % NX
    dz = ((dzi + 1) // 2) * (2 * (dzi % 2) - 1)
    return dx, dz


def kernel(
    mixing_hbm, density_hbm, routes_hbm, weight_hbm, adjoint_hbm,
    gate, incr,
    mixing, density, target, weight, adjoint, pair_of,
    slopes, parts, onehot, prefix, ranks1h, lhs, out_blocks,
    partial, rs1, rs2, final, back, cols, restored, got,
    in_sem, a2a_send, a2a_recv, bk_send, bk_recv,
    rs1_send, rs1_recv, rs2_send, rs2_recv, ag1_send, ag1_recv, ag2_send, ag2_recv,
):
    tile = lax.axis_index("tile")
    lev = lax.axis_index("lev")
    core = tile % NC
    zz = (tile // NC) % NZ
    xx = tile // (NC * NZ)
    right = (lev + 1) % LEVS
    left = (lev + 3) % LEVS
    across = (lev + 2) % LEVS

    def pair_plus(kp):
        dx, dz = shift_of(kp)
        return ((xx + dx) % NX) * NZ + (zz + dz + NZ) % NZ

    def pair_minus(kp):
        dx, dz = shift_of(kp)
        return ((xx - dx + NX) % NX) * NZ + (zz - dz + NZ) % NZ

    loads = [
        pltpu.make_async_copy(weight_hbm.at[0], weight, in_sem.at[0]),
        pltpu.make_async_copy(adjoint_hbm, adjoint, in_sem.at[1]),
        pltpu.make_async_copy(routes_hbm, target, in_sem.at[2]),
        pltpu.make_async_copy(density_hbm, density, in_sem.at[3]),
        pltpu.make_async_copy(mixing_hbm, mixing, in_sem.at[4]),
    ]
    for load in loads:
        load.start()

    barrier = pltpu.get_barrier_semaphore()

    @pl.loop(1, TILES)
    def _(k):
        pl.semaphore_signal(
            barrier, inc=1, device_id={"tile": (tile + k) % TILES}, device_id_type=MESH
        )

    for peer in (left, right):
        pl.semaphore_signal(barrier, inc=1, device_id={"lev": peer}, device_id_type=MESH)

    loads[0].wait()
    mine = weight[:, :GR]
    for k in range(1, LEVS):
        mine = jnp.where(lev == k, weight[:, GR * k : GR * (k + 1)], mine)
    mine_hi, mine_lo = split2(mine)
    rows_hi, rows_lo = split2(mine.T)
    rows3 = jnp.concatenate([rows_hi, rows_hi, rows_lo], axis=1)
    loads[1].wait()

    @pl.loop(0, PAIRS, unroll=4)
    def _(kp):
        at = pl.multiple_of(pair_plus(kp) * 2 * CAP, 2 * CAP)
        g_hi, g_lo = split2(adjoint[:, pl.ds(at, 2 * CAP)])
        part = dot(mine_hi, g_hi) + dot(mine_hi, g_lo) + dot(mine_lo, g_hi)
        for k in range(LEVS):
            for c in range(NC):
                partial[k, kp * NC + c] = part[LD * k : LD * (k + 1), CAP * c : CAP * (c + 1)]

    pl.semaphore_wait(barrier, TILES - 1 + 2)

    def lev_copy(src, dst, send, recv, peer):
        return pltpu.make_async_remote_copy(
            src_ref=src, dst_ref=dst, send_sem=send, recv_sem=recv,
            device_id={"lev": peer}, device_id_type=MESH,
        )

    def rs1_copy(c, way):
        at = c * PC + way * HALF
        return lev_copy(
            partial.at[across, pl.ds(at * NC, HALF * NC)], rs1.at[way, c],
            rs1_send.at[way, c], rs1_recv.at[way, c], (right, left)[way],
        )

    def rs2_copy(c, way):
        peer = (right, left)[way]
        return lev_copy(
            partial.at[peer, pl.ds(c * PC * NC, PC * NC)], rs2.at[way, c],
            rs2_send.at[way, c], rs2_recv.at[way, c], peer,
        )

    def ag1_copy(c, way):
        here = cols.at[lev, pl.ds(c * PC * NC, PC * NC)]
        return lev_copy(
            here, here, ag1_send.at[way, c], ag1_recv.at[way, c], (right, left)[way]
        )

    def ag2_copy(c, way):
        here = cols.at[(left, right)[way], pl.ds((c * PC + way * HALF) * NC, HALF * NC)]
        return lev_copy(
            here, here, ag2_send.at[way, c], ag2_recv.at[way, c], (right, left)[way]
        )

    def rs_first(c):
        for way in range(2):
            rs1_copy(c, way).start()

    def rs_second(c):
        for way in range(2):
            rs1_copy(c, way).wait_recv()
            peer = (right, left)[way]
            at = pl.ds((c * PC + way * HALF) * NC, HALF * NC)
            partial[peer, at] = partial[peer, at] + rs1[way, c]
        for way in range(2):
            rs2_copy(c, way).start()

    def back_copy(kp, c, cs):
        return pltpu.make_async_remote_copy(
            src_ref=final.at[kp * NC + cs], dst_ref=back.at[kp * NC + core],
            send_sem=bk_send, recv_sem=bk_recv.at[c],
            device_id={"tile": pair_plus(kp) * NC + cs}, device_id_type=MESH,
        )

    def out_copy(kp, c, cd):
        return pltpu.make_async_remote_copy(
            src_ref=out_blocks.at[kp * NC + cd], dst_ref=cols.at[lev, kp * NC + core],
            send_sem=a2a_send, recv_sem=a2a_recv.at[c],
            device_id={"tile": pair_minus(kp) * NC + cd}, device_id_type=MESH,
        )

    def exchange(copy_of, c):
        if c == 0:
            copy_of(0, 0, 1 - core).start()

        @pl.loop(c * PC + (1 if c == 0 else 0), (c + 1) * PC)
        def _(kp):
            for other in range(NC):
                copy_of(kp, c, other).start()

    def blocks(buf, count, send, recv):
        some = buf.at[pl.ds(0, count)]
        return pltpu.make_async_remote_copy(
            src_ref=some, dst_ref=some, send_sem=send, recv_sem=recv,
            device_id={"lev": right}, device_id_type=MESH,
        )

    def in_chunk(c):
        return PC * NC - (1 if c == 0 else 0)

    def rs_final(c):
        for way in range(2):
            rs2_copy(c, way).wait_recv()
        at = pl.ds(c * PC * NC, PC * NC)
        final[at] = partial[lev, at] + rs2[0, c] + rs2[1, c]

    for c in range(CHUNKS):
        rs_first(c)

    loads[2].wait()
    for j in range(COLS // CAP):
        names = lax.broadcasted_iota(jnp.int32, (TILES, CAP), 0)
        onehot[TILES * j : TILES * (j + 1), :] = jnp.where(
            target[:, CAP * j : CAP * (j + 1)] == names, 1.0, 0.0
        ).astype(BF16)
    upto = jnp.where(
        lax.broadcasted_iota(jnp.int32, (CAP, 2 * CAP), 0)
        < lax.broadcasted_iota(jnp.int32, (CAP, 2 * CAP), 1),
        1.0, 0.0,
    ).astype(BF16)
    prefix[...] = dot(onehot[...], upto)
    carry = jnp.zeros((TILES, CAP), F32)
    slot = lax.broadcasted_iota(jnp.int32, (NC * CAP, CAP), 0).astype(F32)
    for j in range(COLS // CAP):
        at = slice(TILES * j, TILES * (j + 1))
        before = onehot[at, :].astype(F32) * (prefix[at, :CAP] + carry)
        odd = (target[:, CAP * j : CAP * (j + 1)] % NC).astype(F32)
        rank = jnp.sum(before, axis=0, keepdims=True) + CAP * odd
        ranks1h[:, CAP * j : CAP * (j + 1)] = jnp.where(rank == slot, 1.0, 0.0).astype(BF16)
        carry = carry + prefix[at, CAP:]

    pair_of[...] = jnp.broadcast_to((target[...] // NC).astype(F32), (LD, COLS)).astype(BF16)

    rs_second(0)

    loads[3].wait()
    loads[4].wait()
    wide = 512

    @pl.loop(0, COLS // wide, unroll=2)
    def _(j):
        at = pl.ds(pl.multiple_of(j * wide, wide), wide)
        dens = density[:, at]
        summed = jnp.zeros((LD, wide), F32)
        for species in range(3):
            mix = mixing[species, :, at]
            powered = coefficients[species] * jnp.exp(exponents[species] * jnp.log(dens * mix))
            summed = summed + powered
            slopes[species, :, at] = exponents[species] * powered / mix
        hi, lo = split2(summed)
        parts[0, :, at] = hi
        parts[1, :, at] = lo

    rs_second(1)

    def scatter(c):
        zero = jnp.zeros((), BF16)
        for i in range(PC):
            pair = pair_minus(c * PC + i)
            named = pair_of[...] == pair.astype(F32).astype(BF16)
            for p in range(2):
                at = (p * PC + i) * LD
                lhs[at : at + LD, :] = jnp.where(named, parts[p], zero)

        both = dot(lhs[...], ranks1h[...], ((1,), (1,)))
        placed = both[: PC * LD] + both[PC * LD :]
        for i in range(PC):
            for cd in range(NC):
                out_blocks[(c * PC + i) * NC + cd] = placed[
                    i * LD : (i + 1) * LD, cd * CAP : (cd + 1) * CAP
                ]
        if c == 0:
            cols[lev, core] = out_blocks[core]

    for c in range(CHUNKS):
        scatter(c)
        exchange(out_copy, c)
        if c < 2:
            rs_second(c + 2)
        else:
            rs_final(c - 2)
    exchange(back_copy, 0)
    exchange(back_copy, 1)

    def ag_first(c):
        blocks(out_blocks, in_chunk(c), a2a_send, a2a_recv.at[c]).wait_recv()
        for way in range(2):
            ag1_copy(c, way).start()

    def ag_second(c):
        for way in range(2):
            ag1_copy(c, way).wait_recv()
        for way in range(2):
            ag2_copy(c, way).start()

    def gates(c):
        for way in range(2):
            ag2_copy(c, way).wait_recv()

        @pl.loop(c * PC, (c + 1) * PC, unroll=4)
        def _(kp):
            both = [cols[:, kp * NC + cs].reshape(LEV, CAP) for cs in range(NC)]
            x_hi, x_lo = split2(jnp.concatenate(both, axis=1))
            at = pl.multiple_of(pair_plus(kp) * 2 * CAP, 2 * CAP)
            gate[:, pl.ds(at, 2 * CAP)] = dot(
                rows3, jnp.concatenate([x_hi, x_lo, x_hi], axis=0)
            )

    def gather(c):
        blocks(final, in_chunk(c), bk_send, bk_recv.at[c]).wait_recv()
        if c == 0:
            back[core] = final[core]
        span = PC * LD
        for i in range(PC):
            two = [back[(c * PC + i) * NC + cd] for cd in range(NC)]
            b_hi, b_lo = split2(jnp.concatenate(two, axis=1))
            got[i * LD : (i + 1) * LD, :] = b_hi
            got[span + i * LD : span + (i + 1) * LD, :] = b_lo

        @pl.loop(0, COLS // wide)
        def _(j):
            at = pl.ds(pl.multiple_of(j * wide, wide), wide)
            twice = dot(got[...], ranks1h[:, at])
            spread = twice[:span] + twice[span:]
            names = jnp.broadcast_to(target[:, at] // NC, (LD, wide))
            if c == 0:
                total = jnp.zeros((LD, wide), F32)
            else:
                total = restored[:, at]
            for i in range(PC):
                mine = spread[i * LD : (i + 1) * LD]
                total = jnp.where(names == pair_minus(c * PC + i), mine, total)
            if c < CHUNKS - 1:
                restored[:, at] = total
            else:
                for species in range(3):
                    incr[species, :, at] = slopes[species, :, at] * total

    ag_first(0)
    rs_final(2)
    exchange(back_copy, 2)
    ag_first(1)
    ag_second(0)
    rs_final(3)
    exchange(back_copy, 3)
    ag_first(2)
    ag_second(1)
    gates(0)
    gather(0)
    ag_first(3)
    ag_second(2)
    gates(1)
    gather(1)
    ag_second(3)
    gates(2)
    gather(2)
    gather(3)
    gates(3)

    for c in range(CHUNKS):
        for way in range(2):
            for copy in (rs1_copy, rs2_copy, ag1_copy, ag2_copy):
                copy(c, way).wait_send()
    blocks(out_blocks, TILES - 1, a2a_send, a2a_recv.at[0]).wait_send()
    blocks(final, TILES - 1, bk_send, bk_recv.at[0]).wait_send()


def store(gate, incr, gate_hbm, incr_hbm, sem):
    copies = [
        pltpu.make_async_copy(gate, gate_hbm, sem.at[0]),
        pltpu.make_async_copy(incr, incr_hbm, sem.at[1]),
    ]
    for copy in copies:
        copy.start()
    for copy in copies:
        copy.wait()


def per_device(mixing, density, routes, beam_weight, gate_adjoint):
    dma = pltpu.SemaphoreType.DMA
    block = (LD, CAP)
    per_way = (2, CHUNKS)
    gate_shape, incr_shape = (GR, TILES * CAP), (3, LD, COLS)
    operands = (
        mixing, density, routes.reshape(1, COLS),
        jnp.swapaxes(beam_weight, 1, 2), gate_adjoint,
    )
    gate, incr = pl.pallas_call(
        kernel,
        out_shape=(pltpu.VMEM(gate_shape, F32), pltpu.VMEM(incr_shape, F32)),
        in_specs=[pl.BlockSpec(memory_space=pl.ANY)] * 5,
        out_specs=[pl.BlockSpec(memory_space=pltpu.VMEM)] * 2,
        scratch_shapes=[
            pltpu.VMEM((3, LD, COLS), F32),
            pltpu.VMEM((LD, COLS), F32),
            pltpu.VMEM((1, COLS), jnp.int32),
            pltpu.VMEM((LEV, GR * LEVS), F32),
            pltpu.VMEM((GR, TILES * CAP), F32),
            pltpu.VMEM((LD, COLS), BF16),
            pltpu.VMEM((3, LD, COLS), F32),
            pltpu.VMEM((2, LD, COLS), BF16),
            pltpu.VMEM((TILES * COLS // CAP, CAP), BF16),
            pltpu.VMEM((TILES * COLS // CAP, 2 * CAP), F32),
            pltpu.VMEM((NC * CAP, COLS), BF16),
            pltpu.VMEM((2 * PC * LD, COLS), BF16),
            pltpu.VMEM((TILES, *block), F32),
            pltpu.VMEM((LEVS, TILES, *block), F32),
            pltpu.VMEM((2, CHUNKS, HALF * NC, *block), F32),
            pltpu.VMEM((2, CHUNKS, PC * NC, *block), F32),
            pltpu.VMEM((TILES, *block), F32),
            pltpu.VMEM((TILES, *block), F32),
            pltpu.VMEM((LEVS, TILES, *block), F32),
            pltpu.VMEM((LD, COLS), F32),
            pltpu.VMEM((2 * PC * LD, NC * CAP), BF16),
            dma((5,)), dma, dma((CHUNKS,)), dma, dma((CHUNKS,)),
            dma(per_way), dma(per_way), dma(per_way), dma(per_way),
            dma(per_way), dma(per_way), dma(per_way), dma(per_way),
        ],
        compiler_params=pltpu.CompilerParams(
            collective_id=0, has_side_effects=True, vmem_limit_bytes=48 * 1024 * 1024
        ),
    )(*[pltpu.with_memory_space_constraint(x, pltpu.HBM) for x in operands])
    return pl.pallas_call(
        store,
        out_shape=(
            jax.ShapeDtypeStruct(gate_shape, F32), jax.ShapeDtypeStruct(incr_shape, F32)
        ),
        in_specs=[pl.BlockSpec(memory_space=pl.ANY)] * 2,
        out_specs=[pl.BlockSpec(memory_space=pl.ANY)] * 2,
        scratch_shapes=[dma((2,))],
    )(*[pltpu.with_memory_space_constraint(x, pltpu.VMEM) for x in (gate, incr)])


def solution(mesh):
    return jax.shard_map(
        per_device,
        mesh=mesh,
        in_specs=(
            P(None, "lev", "tile"),
            P("lev", "tile"),
            P("tile", None),
            P("tile", None, None),
            P("lev", "tile"),
        ),
        out_specs=(P("lev", "tile"), P(None, "lev", "tile")),
        check_vma=False,
    )
```

```python
import jax
import jax.numpy as jnp
from jax import lax
from jax.experimental import pallas as pl
from jax.experimental.pallas import tpu as pltpu
from jax.sharding import PartitionSpec as P

coefficients = (3.63, 0.96, 1.98)
exponents = (1.75, 1.66, 1.75)

MESH = pl.DeviceIdType.MESH
F32 = jnp.float32
BF16 = jnp.bfloat16

NX, NZ, NC = 4, 8, 2
LEVS = 4
TILES = NX * NZ * NC
PAIRS = NX * NZ
SC = 8
RC = 4
AC = 4
COLS = 4096
LD = 16
LEV = 64
CAP = 128
GR = 42


def split2(value):
    hi = value.astype(BF16)
    lo = (value - hi.astype(F32)).astype(BF16)
    return hi, lo


def dot(a, b, dims=((1,), (0,))):
    return lax.dot_general(a, b, (dims, ((), ())), preferred_element_type=F32)


def shift_of(kp):
    dzi = kp // NX
    dx = kp % NX
    dz = ((dzi + 1) // 2) * (2 * (dzi % 2) - 1)
    return dx, dz


def kernel(
    mixing_hbm, density_hbm, routes_hbm, weight_hbm, adjoint_hbm,
    gate, incr,
    mixing, density, target, weight, adjoint, pair_of,
    slopes, parts, onehot, prefix, ranks1h, lhs, out_blocks,
    partial, rs1, rs2, final, back, cols, restored, got, rows3,
    in_sem, adj_sem, a2a_send, a2a_recv, bk_send, bk_recv,
    rs1_send, rs1_recv, rs2_send, rs2_recv, ag1_send, ag1_recv, ag2_send, ag2_recv, met,
):
    tile = lax.axis_index("tile")
    lev = lax.axis_index("lev")
    core = tile % NC
    zz = (tile // NC) % NZ
    xx = tile // (NC * NZ)
    right = (lev + 1) % LEVS
    left = (lev + 3) % LEVS
    across = (lev + 2) % LEVS

    def pair_plus(kp):
        dx, dz = shift_of(kp)
        return ((xx + dx) % NX) * NZ + (zz + dz + NZ) % NZ

    def pair_minus(kp):
        dx, dz = shift_of(kp)
        return ((xx - dx + NX) % NX) * NZ + (zz - dz + NZ) % NZ

    loads = [
        pltpu.make_async_copy(weight_hbm.at[0], weight, in_sem.at[0]),
        pltpu.make_async_copy(routes_hbm, target, in_sem.at[1]),
        pltpu.make_async_copy(density_hbm, density, in_sem.at[2]),
        pltpu.make_async_copy(mixing_hbm, mixing, in_sem.at[3]),
    ]
    loads[0].start()

    def adjoint_load(c):
        for kp in range(c * SC, (c + 1) * SC):
            at = pl.ds(pl.multiple_of(pair_plus(kp) * NC * CAP, NC * CAP), NC * CAP)
            pltpu.make_async_copy(
                adjoint_hbm.at[:, at], adjoint.at[:, at], adj_sem.at[c]
            ).start()

    adjoint_load(0)

    def adjoint_wait(c):
        some = pl.ds(0, SC * NC * CAP)
        pltpu.make_async_copy(
            adjoint_hbm.at[:, some], adjoint.at[:, some], adj_sem.at[c]
        ).wait()

    def named(dx, dz, dc):
        x, z = (xx + dx + NX) % NX, (zz + dz + NZ) % NZ
        return {"tile": (x * NZ + z) * NC + (core + dc) % NC}

    near_z = [named(0, 1, 0), named(0, -1, 0)]
    near_x = [named(1, 0, 0), named(-1, 0, 0)]
    far_z = [named(0, 2, 0), named(0, -2, 0)]
    far_x = [named(2, 0, 0)]
    twin = [named(0, 0, 1)]

    def tell(sem, peers):
        for peer in peers:
            pl.semaphore_signal(sem, inc=1, device_id=peer, device_id_type=MESH)

    barrier = pltpu.get_barrier_semaphore()
    tell(barrier, [{"lev": left}, {"lev": right}] + near_z + near_x + twin)
    stages = [
        (met.at[0], near_z + near_x),
        (met.at[1], far_z),
        (met.at[2], near_x + far_x),
        (met.at[3], twin),
    ]

    def pass_on(stage):
        if stage > 0:
            sem, peers = stages[stage - 1]
            pl.semaphore_wait(sem, len(peers))
        if stage < len(stages):
            tell(*stages[stage])

    loads[0].wait()
    for c in range(1, PAIRS // SC):
        adjoint_load(c)
    for load in loads[1:]:
        load.start()
    mine = weight[:, :GR]
    for k in range(1, LEVS):
        mine = jnp.where(lev == k, weight[:, GR * k : GR * (k + 1)], mine)
    mine_hi, mine_lo = split2(mine)
    def adjoint_pair(kp):
        at = pl.multiple_of(pair_plus(kp) * 2 * CAP, 2 * CAP)
        g_hi, g_lo = split2(adjoint[:, pl.ds(at, 2 * CAP)])
        part = dot(mine_hi, g_hi) + dot(mine_hi, g_lo) + dot(mine_lo, g_hi)
        for k in range(LEVS):
            for c in range(NC):
                partial[k, kp * NC + c] = part[LD * k : LD * (k + 1), CAP * c : CAP * (c + 1)]

    def lev_copy(src, dst, send, recv, peer):
        return pltpu.make_async_remote_copy(
            src_ref=src, dst_ref=dst, send_sem=send, recv_sem=recv,
            device_id={"lev": peer}, device_id_type=MESH,
        )

    def blocks(buf, count, send, recv):
        some = buf.at[pl.ds(0, count)]
        return pltpu.make_async_remote_copy(
            src_ref=some, dst_ref=some, send_sem=send, recv_sem=recv,
            device_id={"lev": right}, device_id_type=MESH,
        )

    def rs1_copy(c, way):
        at = (c * RC + way * (RC // 2)) * NC
        return lev_copy(
            partial.at[across, pl.ds(at, RC // 2 * NC)], rs1.at[way, c],
            rs1_send, rs1_recv.at[c], (right, left)[way],
        )

    def rs2_copy(c, way):
        peer = (right, left)[way]
        return lev_copy(
            partial.at[peer, pl.ds(c * RC * NC, RC * NC)], rs2.at[way, c],
            rs2_send, rs2_recv.at[c], peer,
        )

    def ag1_copy(c, way):
        here = cols.at[lev, pl.ds(c * AC * NC, AC * NC)]
        return lev_copy(
            here, here, ag1_send, ag1_recv.at[c], (right, left)[way]
        )

    def ag2_copy(c, way):
        at = (c * AC + way * (AC // 2)) * NC
        here = cols.at[(left, right)[way], pl.ds(at, AC // 2 * NC)]
        return lev_copy(
            here, here, ag2_send, ag2_recv.at[c], (right, left)[way]
        )

    def adjoint_sums(c):
        for kp in range(c * RC, (c + 1) * RC):
            adjoint_pair(kp)

    def rs_first(c):
        for way in range(2):
            rs1_copy(c, way).start()

    def rs_second(c):
        blocks(final, RC * NC, rs1_send, rs1_recv.at[c]).wait_recv()
        for way in range(2):
            peer = (right, left)[way]
            at = pl.ds((c * RC + way * (RC // 2)) * NC, RC // 2 * NC)
            partial[peer, at] = partial[peer, at] + rs1[way, c]
        for way in range(2):
            rs2_copy(c, way).start()

    def back_copy(kp, cs):
        return pltpu.make_async_remote_copy(
            src_ref=final.at[kp * NC + cs], dst_ref=back.at[kp * NC + core],
            send_sem=bk_send, recv_sem=bk_recv.at[kp // SC],
            device_id={"tile": pair_plus(kp) * NC + cs}, device_id_type=MESH,
        )

    def out_copy(kp, cd):
        return pltpu.make_async_remote_copy(
            src_ref=out_blocks.at[kp * NC + cd], dst_ref=cols.at[lev, kp * NC + core],
            send_sem=a2a_send, recv_sem=a2a_recv.at[kp // AC],
            device_id={"tile": pair_minus(kp) * NC + cd}, device_id_type=MESH,
        )

    def exchange(copy_of, first, count):
        if first == 0:
            copy_of(0, 1 - core).start()

        @pl.loop(max(first, 1), first + count, unroll=4)
        def _(kp):
            for other in range(NC):
                copy_of(kp, other).start()

    def in_chunk(pairs, c):
        return pairs * NC - (1 if c == 0 else 0)

    def rs_final(c):
        blocks(final, 2 * RC * NC, rs2_send, rs2_recv.at[c]).wait_recv()
        at = pl.ds(c * RC * NC, RC * NC)
        final[at] = partial[lev, at] + rs2[0, c] + rs2[1, c]

    adjoint_wait(0)
    adjoint_sums(0)
    pl.semaphore_wait(barrier, 7)
    pass_on(0)
    rs_first(0)
    for c in range(1, PAIRS // RC):
        if c * RC % SC == 0:
            adjoint_wait(c * RC // SC)
        adjoint_sums(c)
        rs_first(c)
        if c == 4:
            pass_on(1)

    loads[1].wait()
    for j in range(COLS // CAP):
        names = lax.broadcasted_iota(jnp.int32, (TILES, CAP), 0)
        onehot[TILES * j : TILES * (j + 1), :] = jnp.where(
            target[:, CAP * j : CAP * (j + 1)] == names, 1.0, 0.0
        ).astype(BF16)
    upto = jnp.where(
        lax.broadcasted_iota(jnp.int32, (CAP, 2 * CAP), 0)
        < lax.broadcasted_iota(jnp.int32, (CAP, 2 * CAP), 1),
        1.0, 0.0,
    ).astype(BF16)
    prefix[...] = dot(onehot[...], upto)
    carry = jnp.zeros((TILES, CAP), F32)
    slot = lax.broadcasted_iota(jnp.int32, (NC * CAP, CAP), 0).astype(F32)
    for j in range(COLS // CAP):
        at = slice(TILES * j, TILES * (j + 1))
        before = onehot[at, :].astype(F32) * (prefix[at, :CAP] + carry)
        odd = (target[:, CAP * j : CAP * (j + 1)] % NC).astype(F32)
        rank = jnp.sum(before, axis=0, keepdims=True) + CAP * odd
        ranks1h[:, CAP * j : CAP * (j + 1)] = jnp.where(rank == slot, 1.0, 0.0).astype(BF16)
        carry = carry + prefix[at, CAP:]

    pair_of[...] = jnp.broadcast_to((target[...] // NC).astype(F32), (LD, COLS)).astype(BF16)

    pass_on(2)

    loads[2].wait()
    loads[3].wait()
    wide = 512

    @pl.loop(0, COLS // wide, unroll=2)
    def _(j):
        at = pl.ds(pl.multiple_of(j * wide, wide), wide)
        dens = density[:, at]
        summed = jnp.zeros((LD, wide), F32)
        for species in range(3):
            mix = mixing[species, :, at]
            powered = coefficients[species] * jnp.exp(exponents[species] * jnp.log(dens * mix))
            summed = summed + powered
            slopes[species, :, at] = exponents[species] * powered / mix
        hi, lo = split2(summed)
        parts[0, :, at] = hi
        parts[1, :, at] = lo


    rows_hi, rows_lo = split2(mine.T)
    rows3[...] = jnp.concatenate([rows_hi, rows_hi, rows_lo], axis=1)

    def build(c):
        zero = jnp.zeros((), BF16)
        for i in range(SC):
            pair = pair_minus(c * SC + i)
            same = pair_of[...] == pair.astype(F32).astype(BF16)
            for p in range(2):
                at = (p * SC + i) * LD
                lhs[at : at + LD, :] = jnp.where(same, parts[p], zero)

    def place(c):
        both = dot(lhs[...], ranks1h[...], ((1,), (1,)))
        placed = both[: SC * LD] + both[SC * LD :]
        for i in range(SC):
            for cd in range(NC):
                out_blocks[(c * SC + i) * NC + cd] = placed[
                    i * LD : (i + 1) * LD, cd * CAP : (cd + 1) * CAP
                ]
        if c == 0:
            cols[lev, core] = out_blocks[core]

    def ag_first(c):
        blocks(out_blocks, in_chunk(AC, c), a2a_send, a2a_recv.at[c]).wait_recv()
        for way in range(2):
            ag1_copy(c, way).start()

    def ag_second(c):
        blocks(final, 2 * AC * NC, ag1_send, ag1_recv.at[c]).wait_recv()
        for way in range(2):
            ag2_copy(c, way).start()

    def gates(c):
        blocks(final, AC * NC, ag2_send, ag2_recv.at[c]).wait_recv()

        @pl.loop(c * AC, (c + 1) * AC, unroll=AC)
        def _(kp):
            both = [cols[:, kp * NC + cs].reshape(LEV, CAP) for cs in range(NC)]
            x_hi, x_lo = split2(jnp.concatenate(both, axis=1))
            at = pl.multiple_of(pair_plus(kp) * 2 * CAP, 2 * CAP)
            gate[:, pl.ds(at, 2 * CAP)] = dot(
                rows3[...], jnp.concatenate([x_hi, x_lo, x_hi], axis=0)
            )

    def gather(c):
        blocks(final, in_chunk(SC, c), bk_send, bk_recv.at[c]).wait_recv()
        if c == 0:
            back[core] = final[core]
        span = SC * LD
        for i in range(SC):
            two = [back[(c * SC + i) * NC + cd] for cd in range(NC)]
            b_hi, b_lo = split2(jnp.concatenate(two, axis=1))
            got[i * LD : (i + 1) * LD, :] = b_hi
            got[span + i * LD : span + (i + 1) * LD, :] = b_lo

        @pl.loop(0, COLS // wide, unroll=2)
        def _(j):
            at = pl.ds(pl.multiple_of(j * wide, wide), wide)
            twice = dot(got[...], ranks1h[:, at])
            spread = twice[:span] + twice[span:]
            names = jnp.broadcast_to(target[:, at] // NC, (LD, wide))
            if c == 0:
                total = jnp.zeros((LD, wide), F32)
            else:
                total = restored[:, at]
            for i in range(SC):
                mine = spread[i * LD : (i + 1) * LD]
                total = jnp.where(names == pair_minus(c * SC + i), mine, total)
            if c < PAIRS // SC - 1:
                restored[:, at] = total
            else:
                for species in range(3):
                    incr[species, :, at] = slopes[species, :, at] * total

    def rs_return(c):
        rs_final(c)
        exchange(back_copy, c * RC, RC)

    rs_second(0)
    pass_on(3)
    build(0)
    rs_second(1)
    place(0)
    rs_second(2)
    pass_on(4)
    exchange(out_copy, 0, SC)
    rs_second(3)
    build(1)
    rs_second(4)
    place(1)
    exchange(out_copy, SC, SC)
    rs_second(5)
    build(2)
    rs_second(6)
    place(2)
    exchange(out_copy, 2 * SC, SC)
    rs_second(7)
    build(3)
    place(3)
    exchange(out_copy, 3 * SC, SC)
    for c in range(5):
        rs_return(c)
    ag_first(0)
    rs_return(5)
    ag_first(1)
    rs_return(6)
    ag_first(2)
    ag_first(3)
    rs_return(7)
    ag_first(4)
    ag_second(0)
    ag_first(5)
    ag_second(1)
    ag_first(6)
    ag_first(7)
    ag_second(2)
    gather(0)
    ag_second(3)
    gates(0)
    ag_second(4)
    gather(1)
    ag_second(5)
    gates(1)
    ag_second(6)
    ag_second(7)
    gather(2)
    gates(2)
    gates(3)
    gates(4)
    gather(3)
    gates(5)
    gates(6)
    gates(7)

    def finish():
        blocks(final, TILES, rs1_send, rs1_recv.at[0]).wait_send()
        blocks(final, TILES, ag2_send, ag2_recv.at[0]).wait_send()
        for sem in (rs2_send, ag1_send):
            both = cols.at[pl.ds(0, 2)]
            lev_copy(both, both, sem, ag1_recv.at[0], right).wait_send()
        blocks(out_blocks, TILES - 1, a2a_send, a2a_recv.at[0]).wait_send()
        blocks(final, TILES - 1, bk_send, bk_recv.at[0]).wait_send()

    finish()


def store(gate, incr, gate_hbm, incr_hbm, sem):
    pieces, wide = 4, TILES * CAP // 4
    copies = []
    for i in range(pieces):
        at = pl.ds(i * wide, wide)
        copies.append(pltpu.make_async_copy(gate.at[:, at], gate_hbm.at[:, at], sem.at[i]))
    for i in range(3):
        copies.append(pltpu.make_async_copy(incr.at[i], incr_hbm.at[i], sem.at[pieces + i]))
    for copy in copies:
        copy.start()
    for copy in copies:
        copy.wait()


def per_device(mixing, density, routes, beam_weight, gate_adjoint):
    dma = pltpu.SemaphoreType.DMA
    block = (LD, CAP)
    rs_way = (2, PAIRS // RC)
    gate_shape, incr_shape = (GR, TILES * CAP), (3, LD, COLS)
    operands = (
        mixing, density, routes.reshape(1, COLS),
        jnp.swapaxes(beam_weight, 1, 2), gate_adjoint,
    )
    gate, incr = pl.pallas_call(
        kernel,
        out_shape=(pltpu.VMEM(gate_shape, F32), pltpu.VMEM(incr_shape, F32)),
        in_specs=[pl.BlockSpec(memory_space=pl.ANY)] * 5,
        out_specs=[pl.BlockSpec(memory_space=pltpu.VMEM)] * 2,
        scratch_shapes=[
            pltpu.VMEM((3, LD, COLS), F32),
            pltpu.VMEM((LD, COLS), F32),
            pltpu.VMEM((1, COLS), jnp.int32),
            pltpu.VMEM((LEV, GR * LEVS), F32),
            pltpu.VMEM((GR, TILES * CAP), F32),
            pltpu.VMEM((LD, COLS), BF16),
            pltpu.VMEM((3, LD, COLS), F32),
            pltpu.VMEM((2, LD, COLS), BF16),
            pltpu.VMEM((TILES * COLS // CAP, CAP), BF16),
            pltpu.VMEM((TILES * COLS // CAP, 2 * CAP), F32),
            pltpu.VMEM((NC * CAP, COLS), BF16),
            pltpu.VMEM((2 * SC * LD, COLS), BF16),
            pltpu.VMEM((TILES, *block), F32),
            pltpu.VMEM((LEVS, TILES, *block), F32),
            pltpu.VMEM((*rs_way, RC // 2 * NC, *block), F32),
            pltpu.VMEM((*rs_way, RC * NC, *block), F32),
            pltpu.VMEM((TILES, *block), F32),
            pltpu.VMEM((TILES, *block), F32),
            pltpu.VMEM((LEVS, TILES, *block), F32),
            pltpu.VMEM((LD, COLS), F32),
            pltpu.VMEM((2 * SC * LD, NC * CAP), BF16),
            pltpu.VMEM((GR, 3 * LEV), BF16),
            dma((4,)), dma((PAIRS // SC,)), dma, dma((PAIRS // AC,)), dma, dma((PAIRS // SC,)),
            dma, dma((PAIRS // RC,)), dma, dma((PAIRS // RC,)),
            dma, dma((PAIRS // AC,)), dma, dma((PAIRS // AC,)),
            pltpu.SemaphoreType.REGULAR((4,)),
        ],
        compiler_params=pltpu.CompilerParams(
            collective_id=0, has_side_effects=True, vmem_limit_bytes=48 * 1024 * 1024
        ),
    )(*[pltpu.with_memory_space_constraint(x, pltpu.HBM) for x in operands])
    return pl.pallas_call(
        store,
        out_shape=(
            jax.ShapeDtypeStruct(gate_shape, F32), jax.ShapeDtypeStruct(incr_shape, F32)
        ),
        in_specs=[pl.BlockSpec(memory_space=pl.ANY)] * 2,
        out_specs=[pl.BlockSpec(memory_space=pl.ANY)] * 2,
        scratch_shapes=[dma((7,))],
    )(*[pltpu.with_memory_space_constraint(x, pltpu.VMEM) for x in (gate, incr)])


def solution(mesh):
    return jax.shard_map(
        per_device,
        mesh=mesh,
        in_specs=(
            P(None, "lev", "tile"),
            P("lev", "tile"),
            P("tile", None),
            P("tile", None, None),
            P("lev", "tile"),
        ),
        out_specs=(P("lev", "tile"), P(None, "lev", "tile")),
        check_vma=False,
    )
```

```python
import jax
import jax.numpy as jnp
from jax import lax
from jax.experimental import pallas as pl
from jax.experimental.pallas import tpu as pltpu
from jax.sharding import PartitionSpec as P

coefficients = (3.63, 0.96, 1.98)
exponents = (1.75, 1.66, 1.75)

MESH = pl.DeviceIdType.MESH
F32 = jnp.float32
BF16 = jnp.bfloat16

NX, NZ, NC = 4, 8, 2
LEVS = 4
TILES = NX * NZ * NC
PAIRS = NX * NZ
SC = 8
QC = 8
RC = 4
AC = 4
OWN = NX
COLS = 4096
LD = 16
LEV = 64
CAP = 128
GR = 42


def split2(value):
    hi = value.astype(BF16)
    lo = (value - hi.astype(F32)).astype(BF16)
    return hi, lo


def dot(a, b, dims=((1,), (0,))):
    return lax.dot_general(a, b, (dims, ((), ())), preferred_element_type=F32)


def shift_of(kp):
    dzi = kp // NX
    dx = kp % NX
    dz = (4 - dzi // 2) * (1 - 2 * (dzi % 2)) + 4 * ((8 - dzi) // 7 - (8 - dzi) // 8)
    return dx, dz


def kernel(
    mixing_hbm, density_hbm, routes_hbm, weight_hbm, adjoint_hbm,
    gate, incr,
    mixing, density, target, weight, adjoint, pair_of,
    slopes, parts, onehot, prefix, ranks1h, lhs, out_blocks,
    partial, rs1, rs2, final, back, cols, restored, got, rows3,
    in_sem, adj_sem, a2a_send, a2a_recv, bk_send, bk_recv,
    rs1_send, rs1_recv, rs2_send, rs2_recv, ag1_send, ag1_recv, ag2_send, ag2_recv, met,
):
    tile = lax.axis_index("tile")
    lev = lax.axis_index("lev")
    core = tile % NC
    zz = (tile // NC) % NZ
    xx = tile // (NC * NZ)
    right = (lev + 1) % LEVS
    left = (lev + 3) % LEVS
    across = (lev + 2) % LEVS

    def pair_plus(kp):
        dx, dz = shift_of(kp)
        return ((xx + dx) % NX) * NZ + (zz + dz + NZ) % NZ

    def pair_minus(kp):
        dx, dz = shift_of(kp)
        return ((xx - dx + NX) % NX) * NZ + (zz - dz + NZ) % NZ

    loads = [
        pltpu.make_async_copy(weight_hbm.at[0], weight, in_sem.at[0]),
        pltpu.make_async_copy(routes_hbm, target, in_sem.at[1]),
        pltpu.make_async_copy(density_hbm, density, in_sem.at[2]),
        pltpu.make_async_copy(mixing_hbm, mixing, in_sem.at[3]),
    ]
    loads[0].start()

    def adjoint_load(c):
        for kp in range(c * SC, (c + 1) * SC):
            at = pl.ds(pl.multiple_of(pair_plus(kp) * NC * CAP, NC * CAP), NC * CAP)
            pltpu.make_async_copy(
                adjoint_hbm.at[:, at], adjoint.at[:, at], adj_sem.at[c]
            ).start()

    adjoint_load(0)

    def adjoint_wait(c):
        some = pl.ds(0, SC * NC * CAP)
        pltpu.make_async_copy(
            adjoint_hbm.at[:, some], adjoint.at[:, some], adj_sem.at[c]
        ).wait()

    def named(dx, dz, dc):
        x, z = (xx + dx + NX) % NX, (zz + dz + NZ) % NZ
        return {"tile": (x * NZ + z) * NC + (core + dc) % NC}

    near = [named(0, 1, 0), named(0, -1, 0), named(1, 0, 0), named(-1, 0, 0)]
    far_z = [named(0, 2, 0), named(0, -2, 0)]
    all_x = [named(1, 0, 0), named(2, 0, 0), named(3, 0, 0)]
    twin_x = [named(1, 0, 1), named(2, 0, 1), named(3, 0, 1)]
    twin = [named(0, 0, 1)]
    first = [{"lev": left}, {"lev": right}] + near + twin

    def tell(sem, peers):
        for peer in peers:
            pl.semaphore_signal(sem, inc=1, device_id=peer, device_id_type=MESH)

    barrier = pltpu.get_barrier_semaphore()
    tell(barrier, first)
    stages = [
        (met.at[0], near),
        (met.at[1], far_z + all_x),
        (met.at[2], all_x + twin_x + twin),
    ]

    def pass_on(stage):
        if stage > 0:
            sem, peers = stages[stage - 1]
            pl.semaphore_wait(sem, len(peers))
        if stage < len(stages):
            tell(*stages[stage])

    loads[0].wait()
    for c in range(1, PAIRS // SC):
        adjoint_load(c)
    for load in loads[1:]:
        load.start()
    mine = weight[:, :GR]
    for k in range(1, LEVS):
        mine = jnp.where(lev == k, weight[:, GR * k : GR * (k + 1)], mine)
    mine_hi, mine_lo = split2(mine)
    def adjoint_pair(kp):
        at = pl.multiple_of(pair_plus(kp) * 2 * CAP, 2 * CAP)
        g_hi, g_lo = split2(adjoint[:, pl.ds(at, 2 * CAP)])
        part = dot(mine_hi, g_hi) + dot(mine_hi, g_lo) + dot(mine_lo, g_hi)
        for k in range(LEVS):
            for c in range(NC):
                partial[k, kp * NC + c] = part[LD * k : LD * (k + 1), CAP * c : CAP * (c + 1)]

    def lev_copy(src, dst, send, recv, peer):
        return pltpu.make_async_remote_copy(
            src_ref=src, dst_ref=dst, send_sem=send, recv_sem=recv,
            device_id={"lev": peer}, device_id_type=MESH,
        )

    def blocks(buf, count, send, recv):
        some = buf.at[pl.ds(0, count)]
        return pltpu.make_async_remote_copy(
            src_ref=some, dst_ref=some, send_sem=send, recv_sem=recv,
            device_id={"lev": right}, device_id_type=MESH,
        )

    def rs1_copy(c, way):
        at = (c * RC + way * (RC // 2)) * NC
        return lev_copy(
            partial.at[across, pl.ds(at, RC // 2 * NC)], rs1.at[way, c],
            rs1_send, rs1_recv.at[c], (right, left)[way],
        )

    def rs2_copy(c, way):
        peer = (right, left)[way]
        return lev_copy(
            partial.at[peer, pl.ds(c * RC * NC, RC * NC)], rs2.at[way, c],
            rs2_send, rs2_recv.at[c], peer,
        )

    def ag1_copy(c, way):
        here = cols.at[lev, pl.ds(c * AC * NC, AC * NC)]
        return lev_copy(
            here, here, ag1_send, ag1_recv.at[c], (right, left)[way]
        )

    def ag2_copy(c, way):
        at = (c * AC + way * (AC // 2)) * NC
        here = cols.at[(left, right)[way], pl.ds(at, AC // 2 * NC)]
        return lev_copy(
            here, here, ag2_send, ag2_recv.at[c], (right, left)[way]
        )

    def adjoint_sums(c):
        for kp in range(c * RC, (c + 1) * RC):
            adjoint_pair(kp)

    def rs_first(c):
        for way in range(2):
            rs1_copy(c, way).start()

    def rs_second(c):
        blocks(final, RC * NC, rs1_send, rs1_recv.at[c]).wait_recv()
        for way in range(2):
            peer = (right, left)[way]
            at = pl.ds((c * RC + way * (RC // 2)) * NC, RC // 2 * NC)
            partial[peer, at] = partial[peer, at] + rs1[way, c]
        for way in range(2):
            rs2_copy(c, way).start()

    def back_copy(kp, cs):
        return pltpu.make_async_remote_copy(
            src_ref=final.at[kp * NC + cs], dst_ref=back.at[kp * NC + core],
            send_sem=bk_send, recv_sem=bk_recv.at[kp // SC],
            device_id={"tile": pair_plus(kp) * NC + cs}, device_id_type=MESH,
        )

    def out_copy(kp, cd):
        return pltpu.make_async_remote_copy(
            src_ref=out_blocks.at[kp * NC + cd], dst_ref=cols.at[lev, kp * NC + core],
            send_sem=a2a_send, recv_sem=a2a_recv.at[kp // AC],
            device_id={"tile": pair_minus(kp) * NC + cd}, device_id_type=MESH,
        )

    def exchange(copy_of, first, count):
        def pairs(at, number):
            @pl.loop(at, at + number, unroll=min(4, number))
            def _(kp):
                for other in range(NC):
                    copy_of(kp, other).start()

        if first <= OWN < first + count:
            if first < OWN:
                pairs(first, OWN - first)
            copy_of(OWN, 1 - core).start()
            pairs(OWN + 1, first + count - OWN - 1)
        else:
            pairs(first, count)

    def in_chunk(pairs, c):
        return pairs * NC - (1 if c == OWN // pairs else 0)

    def rs_final(c):
        blocks(final, 2 * RC * NC, rs2_send, rs2_recv.at[c]).wait_recv()
        at = pl.ds(c * RC * NC, RC * NC)
        final[at] = partial[lev, at] + rs2[0, c] + rs2[1, c]

    adjoint_wait(0)
    adjoint_sums(0)
    pl.semaphore_wait(barrier, len(first))
    pass_on(0)
    rs_first(0)
    for c in range(1, PAIRS // RC):
        if c * RC % SC == 0:
            adjoint_wait(c * RC // SC)
        adjoint_sums(c)
        rs_first(c)
    pass_on(1)

    loads[1].wait()
    for j in range(COLS // CAP):
        names = lax.broadcasted_iota(jnp.int32, (TILES, CAP), 0)
        onehot[TILES * j : TILES * (j + 1), :] = jnp.where(
            target[:, CAP * j : CAP * (j + 1)] == names, 1.0, 0.0
        ).astype(BF16)
    upto = jnp.where(
        lax.broadcasted_iota(jnp.int32, (CAP, 2 * CAP), 0)
        < lax.broadcasted_iota(jnp.int32, (CAP, 2 * CAP), 1),
        1.0, 0.0,
    ).astype(BF16)
    prefix[...] = dot(onehot[...], upto)
    carry = jnp.zeros((TILES, CAP), F32)
    slot = lax.broadcasted_iota(jnp.int32, (NC * CAP, CAP), 0).astype(F32).astype(BF16)
    one, zero = jnp.ones((), BF16), jnp.zeros((), BF16)
    for j in range(COLS // CAP):
        at = slice(TILES * j, TILES * (j + 1))
        before = onehot[at, :].astype(F32) * (prefix[at, :CAP] + carry)
        odd = (target[:, CAP * j : CAP * (j + 1)] % NC).astype(F32)
        rank = jnp.sum(before, axis=0, keepdims=True) + CAP * odd
        ranks1h[:, CAP * j : CAP * (j + 1)] = jnp.where(
            jnp.broadcast_to(rank.astype(BF16), slot.shape) == slot, one, zero
        )
        carry = carry + prefix[at, CAP:]

    pair_of[...] = jnp.broadcast_to((target[...] // NC).astype(F32), (LD, COLS)).astype(BF16)


    loads[2].wait()
    loads[3].wait()
    wide = 512

    @pl.loop(0, COLS // wide, unroll=2)
    def _(j):
        at = pl.ds(pl.multiple_of(j * wide, wide), wide)
        dens = density[:, at]
        summed = jnp.zeros((LD, wide), F32)
        for species in range(3):
            mix = mixing[species, :, at]
            powered = coefficients[species] * jnp.exp(exponents[species] * jnp.log(dens * mix))
            summed = summed + powered
            slopes[species, :, at] = exponents[species] * powered / mix
        hi, lo = split2(summed)
        parts[0, :, at] = hi
        parts[1, :, at] = lo


    rows_hi, rows_lo = split2(mine.T)
    rows3[...] = jnp.concatenate([rows_hi, rows_hi, rows_lo], axis=1)

    def build(c):
        for i in range(SC):
            pair = pair_minus(c * SC + i)
            same = pair_of[...] == pair.astype(F32).astype(BF16)
            for p in range(2):
                at = (i // QC * 2 * QC + p * QC + i % QC) * LD
                lhs[at : at + LD, :] = jnp.where(same, parts[p], zero)

    def place(c):
        for q in range(SC // QC):
            rows = 2 * QC * LD
            both = dot(lhs[q * rows : (q + 1) * rows], ranks1h[...], ((1,), (1,)))
            placed = both[: QC * LD] + both[QC * LD :]
            for i in range(QC):
                for cd in range(NC):
                    out_blocks[(c * SC + q * QC + i) * NC + cd] = placed[
                        i * LD : (i + 1) * LD, cd * CAP : (cd + 1) * CAP
                    ]
        if c == OWN // SC:
            cols[lev, OWN * NC + core] = out_blocks[OWN * NC + core]

    def ag_first(c):
        blocks(out_blocks, in_chunk(AC, c), a2a_send, a2a_recv.at[c]).wait_recv()
        for way in range(2):
            ag1_copy(c, way).start()

    def ag_second(c):
        blocks(final, 2 * AC * NC, ag1_send, ag1_recv.at[c]).wait_recv()
        for way in range(2):
            ag2_copy(c, way).start()

    def gates(c):
        blocks(final, AC * NC, ag2_send, ag2_recv.at[c]).wait_recv()

        @pl.loop(c * AC, (c + 1) * AC, unroll=AC)
        def _(kp):
            both = [cols[:, kp * NC + cs].reshape(LEV, CAP) for cs in range(NC)]
            x_hi, x_lo = split2(jnp.concatenate(both, axis=1))
            at = pl.multiple_of(pair_plus(kp) * 2 * CAP, 2 * CAP)
            gate[:, pl.ds(at, 2 * CAP)] = dot(
                rows3[...], jnp.concatenate([x_hi, x_lo, x_hi], axis=0)
            )

    def gather(c):
        blocks(final, in_chunk(SC, c), bk_send, bk_recv.at[c]).wait_recv()
        if c == OWN // SC:
            back[OWN * NC + core] = final[OWN * NC + core]
        span = SC * LD
        for i in range(SC):
            two = [back[(c * SC + i) * NC + cd] for cd in range(NC)]
            b_hi, b_lo = split2(jnp.concatenate(two, axis=1))
            got[i * LD : (i + 1) * LD, :] = b_hi
            got[span + i * LD : span + (i + 1) * LD, :] = b_lo

        @pl.loop(0, COLS // wide, unroll=4)
        def _(j):
            at = pl.ds(pl.multiple_of(j * wide, wide), wide)
            twice = dot(got[...], ranks1h[:, at])
            spread = twice[:span] + twice[span:]
            names = jnp.broadcast_to(target[:, at] // NC, (LD, wide))
            if c == 0:
                total = jnp.zeros((LD, wide), F32)
            else:
                total = restored[:, at]
            for i in range(SC):
                mine = spread[i * LD : (i + 1) * LD]
                total = jnp.where(names == pair_minus(c * SC + i), mine, total)
            if c < PAIRS // SC - 1:
                restored[:, at] = total
            else:
                for species in range(3):
                    incr[species, :, at] = slopes[species, :, at] * total

    def rs_return(c):
        rs_final(c)
        exchange(back_copy, c * RC, RC)

    pass_on(2)
    rs_second(0)
    build(0)
    rs_second(1)
    place(0)
    rs_second(2)
    pass_on(3)
    exchange(out_copy, 0, SC)
    rs_second(3)
    build(1)
    rs_second(4)
    place(1)
    exchange(out_copy, SC, SC)
    rs_second(5)
    build(2)
    rs_second(6)
    place(2)
    exchange(out_copy, 2 * SC, SC)
    rs_second(7)
    build(3)
    place(3)
    exchange(out_copy, 3 * SC, SC)
    for c in range(5):
        rs_return(c)
    ag_first(0)
    rs_return(5)
    ag_first(1)
    rs_return(6)
    ag_first(2)
    ag_first(3)
    rs_return(7)
    ag_first(4)
    ag_second(0)
    ag_first(5)
    ag_second(1)
    ag_first(6)
    ag_first(7)
    ag_second(2)
    ag_second(3)
    ag_second(4)
    gather(0)
    ag_second(5)
    gates(0)
    ag_second(6)
    gather(1)
    ag_second(7)
    gates(1)
    gather(2)
    gates(2)
    gates(3)
    gather(3)
    gates(4)
    gates(5)
    gates(6)
    gates(7)

    def finish():
        blocks(final, TILES, rs1_send, rs1_recv.at[0]).wait_send()
        blocks(final, TILES, ag2_send, ag2_recv.at[0]).wait_send()
        for sem in (rs2_send, ag1_send):
            both = cols.at[pl.ds(0, 2)]
            lev_copy(both, both, sem, ag1_recv.at[0], right).wait_send()
        blocks(out_blocks, TILES - 1, a2a_send, a2a_recv.at[0]).wait_send()
        blocks(final, TILES - 1, bk_send, bk_recv.at[0]).wait_send()

    finish()


def store(gate, incr, gate_hbm, incr_hbm, sem):
    pieces, wide = 4, TILES * CAP // 4
    copies = []
    for i in range(pieces):
        at = pl.ds(i * wide, wide)
        copies.append(pltpu.make_async_copy(gate.at[:, at], gate_hbm.at[:, at], sem.at[i]))
    for i in range(3):
        copies.append(pltpu.make_async_copy(incr.at[i], incr_hbm.at[i], sem.at[pieces + i]))
    for copy in copies:
        copy.start()
    for copy in copies:
        copy.wait()


def per_device(mixing, density, routes, beam_weight, gate_adjoint):
    dma = pltpu.SemaphoreType.DMA
    block = (LD, CAP)
    rs_way = (2, PAIRS // RC)
    gate_shape, incr_shape = (GR, TILES * CAP), (3, LD, COLS)
    operands = (
        mixing, density, routes.reshape(1, COLS),
        jnp.swapaxes(beam_weight, 1, 2), gate_adjoint,
    )
    gate, incr = pl.pallas_call(
        kernel,
        out_shape=(pltpu.VMEM(gate_shape, F32), pltpu.VMEM(incr_shape, F32)),
        in_specs=[pl.BlockSpec(memory_space=pl.ANY)] * 5,
        out_specs=[pl.BlockSpec(memory_space=pltpu.VMEM)] * 2,
        scratch_shapes=[
            pltpu.VMEM((3, LD, COLS), F32),
            pltpu.VMEM((LD, COLS), F32),
            pltpu.VMEM((1, COLS), jnp.int32),
            pltpu.VMEM((LEV, GR * LEVS), F32),
            pltpu.VMEM((GR, TILES * CAP), F32),
            pltpu.VMEM((LD, COLS), BF16),
            pltpu.VMEM((3, LD, COLS), F32),
            pltpu.VMEM((2, LD, COLS), BF16),
            pltpu.VMEM((TILES * COLS // CAP, CAP), BF16),
            pltpu.VMEM((TILES * COLS // CAP, 2 * CAP), F32),
            pltpu.VMEM((NC * CAP, COLS), BF16),
            pltpu.VMEM((2 * SC * LD, COLS), BF16),
            pltpu.VMEM((TILES, *block), F32),
            pltpu.VMEM((LEVS, TILES, *block), F32),
            pltpu.VMEM((*rs_way, RC // 2 * NC, *block), F32),
            pltpu.VMEM((*rs_way, RC * NC, *block), F32),
            pltpu.VMEM((TILES, *block), F32),
            pltpu.VMEM((TILES, *block), F32),
            pltpu.VMEM((LEVS, TILES, *block), F32),
            pltpu.VMEM((LD, COLS), F32),
            pltpu.VMEM((2 * SC * LD, NC * CAP), BF16),
            pltpu.VMEM((GR, 3 * LEV), BF16),
            dma((4,)), dma((PAIRS // SC,)), dma, dma((PAIRS // AC,)), dma, dma((PAIRS // SC,)),
            dma, dma((PAIRS // RC,)), dma, dma((PAIRS // RC,)),
            dma, dma((PAIRS // AC,)), dma, dma((PAIRS // AC,)),
            pltpu.SemaphoreType.REGULAR((3,)),
        ],
        compiler_params=pltpu.CompilerParams(
            collective_id=0, has_side_effects=True, vmem_limit_bytes=48 * 1024 * 1024
        ),
    )(*[pltpu.with_memory_space_constraint(x, pltpu.HBM) for x in operands])
    return pl.pallas_call(
        store,
        out_shape=(
            jax.ShapeDtypeStruct(gate_shape, F32), jax.ShapeDtypeStruct(incr_shape, F32)
        ),
        in_specs=[pl.BlockSpec(memory_space=pl.ANY)] * 2,
        out_specs=[pl.BlockSpec(memory_space=pl.ANY)] * 2,
        scratch_shapes=[dma((7,))],
    )(*[pltpu.with_memory_space_constraint(x, pltpu.VMEM) for x in (gate, incr)])


def solution(mesh):
    return jax.shard_map(
        per_device,
        mesh=mesh,
        in_specs=(
            P(None, "lev", "tile"),
            P("lev", "tile"),
            P("tile", None),
            P("tile", None, None),
            P("lev", "tile"),
        ),
        out_specs=(P("lev", "tile"), P(None, "lev", "tile")),
        check_vma=False,
    )
```

```python
import jax
import jax.numpy as jnp
from jax import lax
from jax.experimental import pallas as pl
from jax.experimental.pallas import tpu as pltpu
from jax.sharding import PartitionSpec as P

coefficients = (3.63, 0.96, 1.98)
exponents = (1.75, 1.66, 1.75)

MESH = pl.DeviceIdType.MESH
F32 = jnp.float32
BF16 = jnp.bfloat16

NX, NZ, NC = 4, 8, 2
LEVS = 4
TILES = NX * NZ * NC
PAIRS = NX * NZ
SC = 8
QC = 8
RC = 4
AC = 4
OWN = NX
COLS = 4096
LD = 16
LEV = 64
CAP = 128
GR = 42


def split2(value):
    hi = value.astype(BF16)
    lo = (value - hi.astype(F32)).astype(BF16)
    return hi, lo


def dot(a, b, dims=((1,), (0,))):
    return lax.dot_general(a, b, (dims, ((), ())), preferred_element_type=F32)


def shift_of(kp):
    dzi = kp // NX
    dx = kp % NX
    dz = (4 - dzi // 2) * (1 - 2 * (dzi % 2)) + 4 * ((8 - dzi) // 7 - (8 - dzi) // 8)
    return dx, dz


def kernel(
    mixing_hbm, density_hbm, routes_hbm, weight_hbm, adjoint_hbm,
    gate, incr,
    mixing, density, target, weight, adjoint, pair_of,
    slopes, parts, onehot, prefix, ranks1h, lhs, out_blocks,
    partial, rs1, rs2, final, back, cols, restored, got, rows3,
    in_sem, adj_sem, a2a_send, a2a_recv, bk_send, bk_recv,
    rs1_send, rs1_recv, rs2_send, rs2_recv, ag1_send, ag1_recv, ag2_send, ag2_recv, met,
):
    tile = lax.axis_index("tile")
    lev = lax.axis_index("lev")
    core = tile % NC
    zz = (tile // NC) % NZ
    xx = tile // (NC * NZ)
    right = (lev + 1) % LEVS
    left = (lev + 3) % LEVS
    across = (lev + 2) % LEVS

    def pair_plus(kp):
        dx, dz = shift_of(kp)
        return ((xx + dx) % NX) * NZ + (zz + dz + NZ) % NZ

    def pair_minus(kp):
        dx, dz = shift_of(kp)
        return ((xx - dx + NX) % NX) * NZ + (zz - dz + NZ) % NZ

    loads = [
        pltpu.make_async_copy(weight_hbm.at[0], weight, in_sem.at[0]),
        pltpu.make_async_copy(routes_hbm, target, in_sem.at[1]),
        pltpu.make_async_copy(density_hbm, density, in_sem.at[2]),
        pltpu.make_async_copy(mixing_hbm, mixing, in_sem.at[3]),
    ]
    loads[0].start()

    def adjoint_load(c):
        for kp in range(c * SC, (c + 1) * SC):
            at = pl.ds(pl.multiple_of(pair_plus(kp) * NC * CAP, NC * CAP), NC * CAP)
            pltpu.make_async_copy(
                adjoint_hbm.at[:, at], adjoint.at[:, at], adj_sem.at[c]
            ).start()

    adjoint_load(0)

    def adjoint_wait(c):
        some = pl.ds(0, SC * NC * CAP)
        pltpu.make_async_copy(
            adjoint_hbm.at[:, some], adjoint.at[:, some], adj_sem.at[c]
        ).wait()

    def named(dx, dz, dc):
        x, z = (xx + dx + NX) % NX, (zz + dz + NZ) % NZ
        return {"tile": (x * NZ + z) * NC + (core + dc) % NC}

    near = [named(0, 1, 0), named(0, -1, 0), named(1, 0, 0), named(-1, 0, 0)]
    far_z = [named(0, 2, 0), named(0, -2, 0)]
    all_x = [named(1, 0, 0), named(2, 0, 0), named(3, 0, 0)]
    twin_x = [named(1, 0, 1), named(2, 0, 1), named(3, 0, 1)]
    twin = [named(0, 0, 1)]
    first = [{"lev": left}, {"lev": right}] + near + twin

    def tell(sem, peers):
        for peer in peers:
            pl.semaphore_signal(sem, inc=1, device_id=peer, device_id_type=MESH)

    barrier = pltpu.get_barrier_semaphore()
    tell(barrier, first)
    stages = [
        (met.at[0], near),
        (met.at[1], far_z + all_x),
        (met.at[2], all_x + twin_x + twin),
    ]

    def pass_on(stage):
        if stage > 0:
            sem, peers = stages[stage - 1]
            pl.semaphore_wait(sem, len(peers))
        if stage < len(stages):
            tell(*stages[stage])

    loads[0].wait()
    for c in range(1, PAIRS // SC):
        adjoint_load(c)
    for load in loads[1:]:
        load.start()
    mine = weight[:, :GR]
    for k in range(1, LEVS):
        mine = jnp.where(lev == k, weight[:, GR * k : GR * (k + 1)], mine)
    mine_hi, mine_lo = split2(mine)
    def adjoint_pair(kp):
        at = pl.multiple_of(pair_plus(kp) * 2 * CAP, 2 * CAP)
        g_hi, g_lo = split2(adjoint[:, pl.ds(at, 2 * CAP)])
        part = dot(mine_hi, g_hi) + dot(mine_hi, g_lo) + dot(mine_lo, g_hi)
        for k in range(LEVS):
            for c in range(NC):
                partial[k, kp * NC + c] = part[LD * k : LD * (k + 1), CAP * c : CAP * (c + 1)]

    def lev_copy(src, dst, send, recv, peer):
        return pltpu.make_async_remote_copy(
            src_ref=src, dst_ref=dst, send_sem=send, recv_sem=recv,
            device_id={"lev": peer}, device_id_type=MESH,
        )

    def blocks(buf, count, send, recv):
        some = buf.at[pl.ds(0, count)]
        return pltpu.make_async_remote_copy(
            src_ref=some, dst_ref=some, send_sem=send, recv_sem=recv,
            device_id={"lev": right}, device_id_type=MESH,
        )

    def rs1_copy(c, way):
        at = (c * RC + way * (RC // 2)) * NC
        return lev_copy(
            partial.at[across, pl.ds(at, RC // 2 * NC)], rs1.at[way, c],
            rs1_send, rs1_recv.at[c], (right, left)[way],
        )

    def rs2_copy(c, way):
        peer = (right, left)[way]
        return lev_copy(
            partial.at[peer, pl.ds(c * RC * NC, RC * NC)], rs2.at[way, c],
            rs2_send, rs2_recv.at[c], peer,
        )

    def ag1_copy(c, way):
        here = cols.at[lev, pl.ds(c * AC * NC, AC * NC)]
        return lev_copy(
            here, here, ag1_send, ag1_recv.at[c], (right, left)[way]
        )

    def ag2_copy(c, way):
        at = (c * AC + way * (AC // 2)) * NC
        here = cols.at[(left, right)[way], pl.ds(at, AC // 2 * NC)]
        return lev_copy(
            here, here, ag2_send, ag2_recv.at[c], (right, left)[way]
        )

    def adjoint_sums(c):
        for kp in range(c * RC, (c + 1) * RC):
            adjoint_pair(kp)

    def rs_first(c):
        for way in range(2):
            rs1_copy(c, way).start()

    def rs_second(c):
        blocks(final, RC * NC, rs1_send, rs1_recv.at[c]).wait_recv()
        for way in range(2):
            peer = (right, left)[way]
            at = pl.ds((c * RC + way * (RC // 2)) * NC, RC // 2 * NC)
            partial[peer, at] = partial[peer, at] + rs1[way, c]
        for way in range(2):
            rs2_copy(c, way).start()

    def back_copy(kp, cs):
        return pltpu.make_async_remote_copy(
            src_ref=final.at[kp * NC + cs], dst_ref=back.at[kp * NC + core],
            send_sem=bk_send, recv_sem=bk_recv.at[kp // SC],
            device_id={"tile": pair_plus(kp) * NC + cs}, device_id_type=MESH,
        )

    def out_copy(kp, cd):
        return pltpu.make_async_remote_copy(
            src_ref=out_blocks.at[kp * NC + cd], dst_ref=cols.at[lev, kp * NC + core],
            send_sem=a2a_send, recv_sem=a2a_recv.at[kp // AC],
            device_id={"tile": pair_minus(kp) * NC + cd}, device_id_type=MESH,
        )

    def exchange(copy_of, first, count):
        for i in range(count):
            kp = first + i % 2 * (count // 2) + i // 2
            if kp == OWN:
                copy_of(kp, 1 - core).start()
            else:
                for other in range(NC):
                    copy_of(kp, other).start()

    def in_chunk(pairs, c):
        return pairs * NC - (1 if c == OWN // pairs else 0)

    def rs_final(c):
        blocks(final, 2 * RC * NC, rs2_send, rs2_recv.at[c]).wait_recv()
        at = pl.ds(c * RC * NC, RC * NC)
        final[at] = partial[lev, at] + rs2[0, c] + rs2[1, c]

    adjoint_wait(0)
    adjoint_sums(0)
    pl.semaphore_wait(barrier, len(first))
    pass_on(0)
    rs_first(0)
    for c in range(1, PAIRS // RC):
        if c * RC % SC == 0:
            adjoint_wait(c * RC // SC)
        adjoint_sums(c)
        rs_first(c)
    pass_on(1)

    loads[1].wait()
    for j in range(COLS // CAP):
        names = lax.broadcasted_iota(jnp.int32, (TILES, CAP), 0)
        onehot[TILES * j : TILES * (j + 1), :] = jnp.where(
            target[:, CAP * j : CAP * (j + 1)] == names, 1.0, 0.0
        ).astype(BF16)
    upto = jnp.where(
        lax.broadcasted_iota(jnp.int32, (CAP, 2 * CAP), 0)
        < lax.broadcasted_iota(jnp.int32, (CAP, 2 * CAP), 1),
        1.0, 0.0,
    ).astype(BF16)
    prefix[...] = dot(onehot[...], upto)
    carry = jnp.zeros((TILES, CAP), F32)
    slot = lax.broadcasted_iota(jnp.int32, (NC * CAP, CAP), 0).astype(F32).astype(BF16)
    one, zero = jnp.ones((), BF16), jnp.zeros((), BF16)
    for j in range(COLS // CAP):
        at = slice(TILES * j, TILES * (j + 1))
        before = onehot[at, :].astype(F32) * (prefix[at, :CAP] + carry)
        odd = (target[:, CAP * j : CAP * (j + 1)] % NC).astype(F32)
        rank = jnp.sum(before, axis=0, keepdims=True) + CAP * odd
        ranks1h[:, CAP * j : CAP * (j + 1)] = jnp.where(
            jnp.broadcast_to(rank.astype(BF16), slot.shape) == slot, one, zero
        )
        carry = carry + prefix[at, CAP:]

    pair_of[...] = jnp.broadcast_to((target[...] // NC).astype(F32), (LD, COLS)).astype(BF16)


    loads[2].wait()
    loads[3].wait()
    wide = 512

    @pl.loop(0, COLS // wide, unroll=2)
    def _(j):
        at = pl.ds(pl.multiple_of(j * wide, wide), wide)
        dens = density[:, at]
        summed = jnp.zeros((LD, wide), F32)
        for species in range(3):
            mix = mixing[species, :, at]
            powered = coefficients[species] * jnp.exp(exponents[species] * jnp.log(dens * mix))
            summed = summed + powered
            slopes[species, :, at] = exponents[species] * powered / mix
        hi, lo = split2(summed)
        parts[0, :, at] = hi
        parts[1, :, at] = lo


    rows_hi, rows_lo = split2(mine.T)
    rows3[...] = jnp.concatenate([rows_hi, rows_hi, rows_lo], axis=1)

    def build(c):
        for i in range(SC):
            pair = pair_minus(c * SC + i)
            same = pair_of[...] == pair.astype(F32).astype(BF16)
            for p in range(2):
                at = (i // QC * 2 * QC + p * QC + i % QC) * LD
                lhs[at : at + LD, :] = jnp.where(same, parts[p], zero)

    def place(c):
        for q in range(SC // QC):
            rows = 2 * QC * LD
            both = dot(lhs[q * rows : (q + 1) * rows], ranks1h[...], ((1,), (1,)))
            placed = both[: QC * LD] + both[QC * LD :]
            for i in range(QC):
                for cd in range(NC):
                    out_blocks[(c * SC + q * QC + i) * NC + cd] = placed[
                        i * LD : (i + 1) * LD, cd * CAP : (cd + 1) * CAP
                    ]
        if c == OWN // SC:
            cols[lev, OWN * NC + core] = out_blocks[OWN * NC + core]

    def ag_first(c):
        blocks(out_blocks, in_chunk(AC, c), a2a_send, a2a_recv.at[c]).wait_recv()
        for way in range(2):
            ag1_copy(c, way).start()

    def ag_second(c):
        blocks(final, 2 * AC * NC, ag1_send, ag1_recv.at[c]).wait_recv()
        for way in range(2):
            ag2_copy(c, way).start()

    def gates(c):
        blocks(final, AC * NC, ag2_send, ag2_recv.at[c]).wait_recv()

        @pl.loop(c * AC, (c + 1) * AC, unroll=AC)
        def _(kp):
            both = [cols[:, kp * NC + cs].reshape(LEV, CAP) for cs in range(NC)]
            x_hi, x_lo = split2(jnp.concatenate(both, axis=1))
            at = pl.multiple_of(pair_plus(kp) * 2 * CAP, 2 * CAP)
            gate[:, pl.ds(at, 2 * CAP)] = dot(
                rows3[...], jnp.concatenate([x_hi, x_lo, x_hi], axis=0)
            )

    def gather(c):
        blocks(final, in_chunk(SC, c), bk_send, bk_recv.at[c]).wait_recv()
        if c == OWN // SC:
            back[OWN * NC + core] = final[OWN * NC + core]
        span = SC * LD
        for i in range(SC):
            two = [back[(c * SC + i) * NC + cd] for cd in range(NC)]
            b_hi, b_lo = split2(jnp.concatenate(two, axis=1))
            got[i * LD : (i + 1) * LD, :] = b_hi
            got[span + i * LD : span + (i + 1) * LD, :] = b_lo

        @pl.loop(0, COLS // wide, unroll=4)
        def _(j):
            at = pl.ds(pl.multiple_of(j * wide, wide), wide)
            twice = dot(got[...], ranks1h[:, at])
            spread = twice[:span] + twice[span:]
            names = jnp.broadcast_to(target[:, at] // NC, (LD, wide))
            if c == 0:
                total = jnp.zeros((LD, wide), F32)
            else:
                total = restored[:, at]
            for i in range(SC):
                mine = spread[i * LD : (i + 1) * LD]
                total = jnp.where(names == pair_minus(c * SC + i), mine, total)
            if c < PAIRS // SC - 1:
                restored[:, at] = total
            else:
                for species in range(3):
                    incr[species, :, at] = slopes[species, :, at] * total

    def rs_return(c):
        rs_final(c)
        exchange(back_copy, c * RC, RC)

    pass_on(2)
    rs_second(0)
    build(0)
    rs_second(1)
    place(0)
    rs_second(2)
    pass_on(3)
    exchange(out_copy, 0, SC)
    rs_second(3)
    build(1)
    rs_second(4)
    place(1)
    exchange(out_copy, SC, SC)
    rs_second(5)
    build(2)
    rs_second(6)
    place(2)
    exchange(out_copy, 2 * SC, SC)
    rs_second(7)
    build(3)
    place(3)
    exchange(out_copy, 3 * SC, SC)
    for c in range(5):
        rs_return(c)
    ag_first(0)
    rs_return(5)
    ag_first(1)
    rs_return(6)
    ag_first(2)
    ag_first(3)
    rs_return(7)
    ag_first(4)
    ag_second(0)
    ag_first(5)
    ag_second(1)
    ag_first(6)
    ag_first(7)
    ag_second(2)
    ag_second(3)
    ag_second(4)
    gather(0)
    ag_second(5)
    gates(0)
    ag_second(6)
    gather(1)
    ag_second(7)
    gates(1)
    gather(2)
    gates(2)
    gates(3)
    gather(3)
    gates(4)
    gates(5)
    gates(6)
    gates(7)

    def finish():
        blocks(final, TILES, rs1_send, rs1_recv.at[0]).wait_send()
        blocks(final, TILES, ag2_send, ag2_recv.at[0]).wait_send()
        for sem in (rs2_send, ag1_send):
            both = cols.at[pl.ds(0, 2)]
            lev_copy(both, both, sem, ag1_recv.at[0], right).wait_send()
        blocks(out_blocks, TILES - 1, a2a_send, a2a_recv.at[0]).wait_send()
        blocks(final, TILES - 1, bk_send, bk_recv.at[0]).wait_send()

    finish()


def store(gate, incr, gate_hbm, incr_hbm, sem):
    pieces, wide = 2, TILES * CAP // 2
    copies = []
    for i in range(pieces):
        at = pl.ds(i * wide, wide)
        copies.append(pltpu.make_async_copy(gate.at[:, at], gate_hbm.at[:, at], sem.at[i]))
    for i in range(3):
        copies.append(pltpu.make_async_copy(incr.at[i], incr_hbm.at[i], sem.at[pieces + i]))
    for copy in copies:
        copy.start()
    for copy in copies:
        copy.wait()


def per_device(mixing, density, routes, beam_weight, gate_adjoint):
    dma = pltpu.SemaphoreType.DMA
    block = (LD, CAP)
    rs_way = (2, PAIRS // RC)
    gate_shape, incr_shape = (GR, TILES * CAP), (3, LD, COLS)
    operands = (
        mixing, density, routes.reshape(1, COLS),
        jnp.swapaxes(beam_weight, 1, 2), gate_adjoint,
    )
    gate, incr = pl.pallas_call(
        kernel,
        out_shape=(pltpu.VMEM(gate_shape, F32), pltpu.VMEM(incr_shape, F32)),
        in_specs=[pl.BlockSpec(memory_space=pl.ANY)] * 5,
        out_specs=[pl.BlockSpec(memory_space=pltpu.VMEM)] * 2,
        scratch_shapes=[
            pltpu.VMEM((3, LD, COLS), F32),
            pltpu.VMEM((LD, COLS), F32),
            pltpu.VMEM((1, COLS), jnp.int32),
            pltpu.VMEM((LEV, GR * LEVS), F32),
            pltpu.VMEM((GR, TILES * CAP), F32),
            pltpu.VMEM((LD, COLS), BF16),
            pltpu.VMEM((3, LD, COLS), F32),
            pltpu.VMEM((2, LD, COLS), BF16),
            pltpu.VMEM((TILES * COLS // CAP, CAP), BF16),
            pltpu.VMEM((TILES * COLS // CAP, 2 * CAP), F32),
            pltpu.VMEM((NC * CAP, COLS), BF16),
            pltpu.VMEM((2 * SC * LD, COLS), BF16),
            pltpu.VMEM((TILES, *block), F32),
            pltpu.VMEM((LEVS, TILES, *block), F32),
            pltpu.VMEM((*rs_way, RC // 2 * NC, *block), F32),
            pltpu.VMEM((*rs_way, RC * NC, *block), F32),
            pltpu.VMEM((TILES, *block), F32),
            pltpu.VMEM((TILES, *block), F32),
            pltpu.VMEM((LEVS, TILES, *block), F32),
            pltpu.VMEM((LD, COLS), F32),
            pltpu.VMEM((2 * SC * LD, NC * CAP), BF16),
            pltpu.VMEM((GR, 3 * LEV), BF16),
            dma((4,)), dma((PAIRS // SC,)), dma, dma((PAIRS // AC,)), dma, dma((PAIRS // SC,)),
            dma, dma((PAIRS // RC,)), dma, dma((PAIRS // RC,)),
            dma, dma((PAIRS // AC,)), dma, dma((PAIRS // AC,)),
            pltpu.SemaphoreType.REGULAR((3,)),
        ],
        compiler_params=pltpu.CompilerParams(
            collective_id=0, has_side_effects=True, vmem_limit_bytes=48 * 1024 * 1024
        ),
    )(*[pltpu.with_memory_space_constraint(x, pltpu.HBM) for x in operands])
    return pl.pallas_call(
        store,
        out_shape=(
            jax.ShapeDtypeStruct(gate_shape, F32), jax.ShapeDtypeStruct(incr_shape, F32)
        ),
        in_specs=[pl.BlockSpec(memory_space=pl.ANY)] * 2,
        out_specs=[pl.BlockSpec(memory_space=pl.ANY)] * 2,
        scratch_shapes=[dma((5,))],
    )(*[pltpu.with_memory_space_constraint(x, pltpu.VMEM) for x in (gate, incr)])


def solution(mesh):
    return jax.shard_map(
        per_device,
        mesh=mesh,
        in_specs=(
            P(None, "lev", "tile"),
            P("lev", "tile"),
            P("tile", None),
            P("tile", None, None),
            P("lev", "tile"),
        ),
        out_specs=(P("lev", "tile"), P(None, "lev", "tile")),
        check_vma=False,
    )
```
